256 devices in a mesh: dp: 64 (over x, z_lo, y), expert: 4 (over z_hi, core).
Axes of the slice: x: 4, y: 4, z: 8 (z_hi: 2, z_lo: 4; z = z_hi * 4 + z_lo), core: 2. Of those that a mesh axis runs over, the one named last changes fastest.
Arguments:
- master: float32 [4, 7168, 2048], P('expert', 'dp'), may hold values from -6 to 6
- first_moment: float32 [4, 7168, 2048], P('expert', 'dp'), may hold values from -0.06 to 0.06
- second_moment: float32 [4, 7168, 2048], P('expert', 'dp'), may hold values from 1e-05 to 0.001
- rotation: int32 [4, 64, 1], replicated, may hold values from 0 to 63; in each aligned block of 64 rows (0 to 63, 64 to 127, ..., all dimensions but the last counted through in order) at most 3 rows name the same one
- assignment: int32 [256], replicated, may hold values from 0 to 255, each once
Outputs:
- saved_master: float32 [4, 256, 3, 448, 128], P('expert', 'dp')
- saved_update: float32 [4, 256, 3, 448, 128], P('expert', 'dp')
- checksums: float32 [4, 2, 256], replicated
The draws below stay inside these ranges and needn't reach their ends.
Inputs may be any that keep to these rules, and one draw needn't show every extreme that they name: rotation[r, j, 0] is the dp index that writes span j of round r; within one round no index is named more than 3 times, and in some round one index is named exactly 3 times. `assignment`: a permutation of the spans' checksum slots.
All inputs are finite; a program needn't handle non-finite values.
Results may differ from the reference program's by a relative error of at most 0.00002.
Values sent between devices are 32-bit elements; how exact they have to be, the bound alone decides.
A program may use at most 64 MiB of HBM per device.

```python
import math
import jax
import jax.numpy as jnp
import numpy as np
from jax import lax

ROWS = 7168
COLS = 2048
LANE = 128
ROUNDS = 4
MOST = 3
STEP = 20
GROUPS = 4
SPANS = 256
N_DP = 64


def block_levels(stream_key, shape, pieces, smallest, top_value):
    gain, own = 1.0, jax.random.fold_in(stream_key, 6)
    for position, blocks in pieces:
        draws = jnp.exp(jax.random.uniform(jax.random.fold_in(own, position), (blocks,), jnp.float32, smallest / len(pieces), top_value / len(pieces)))
        gain = gain * jnp.repeat(draws, shape[position] // blocks).reshape([-1 if axis == position else 1 for axis in range(len(shape))])
    return gain


def shared_out(key, own, number, rows, count, top, bound, slope):
    ranking = jax.random.permutation(key, count)
    packed, usual = shares(count, rows * top, bound, slope, True), shares(count, rows * top, bound, slope, False)
    places = jnp.arange(count)

    def named(tallies, turn):
        used = int((tallies > 0).sum())
        fixed = max(1, used // 4)
        shifted = fixed + (places - fixed + turn * (used - fixed)) % max(1, count - fixed)
        return jnp.zeros((count,), jnp.int32).at[ranking[jnp.where(places < fixed, places, shifted)]].set(jnp.asarray(tallies, jnp.int32))

    tallies = jnp.where(number % 4 == 0, named(packed, number // 4), named(usual, number - number // 4 - 1))
    mixed = jax.random.permutation(jax.random.fold_in(own, 3), count)
    donor, sink = mixed[0:count // 2 * 2:2], mixed[1:count // 2 * 2:2]
    slack = jnp.minimum(tallies[donor] - 1, bound - tallies[sink]) // 2
    slack = jnp.where((donor == ranking[0]) | (sink == ranking[0]) | (tallies[sink] == 0), 0, jnp.maximum(slack, 0))
    shifted = jax.random.randint(jax.random.fold_in(own, 4), (count // 2,), 0, 1 << 20) % (slack + 1)
    tallies = tallies.at[donor].add(-shifted).at[sink].add(shifted)
    items = jnp.searchsorted(jnp.cumsum(tallies), jnp.arange(rows * top), side="right").astype(jnp.int32)
    listing = items.reshape(top, rows).T
    listing = listing[jax.random.permutation(jax.random.fold_in(own, 1), rows)]
    turn = jax.random.randint(jax.random.fold_in(own, 2), (rows, 1), 0, top)
    return jnp.take_along_axis(listing, (jnp.arange(top)[None, :] + turn) % top, axis=1)


def shares(amount, total, reach, slope, full):
    weights = [(1 << 20) // math.isqrt(standing ** slope) + 1 for standing in range(1, amount + 1)]
    largest = reach if full else min(reach, max(-(-total // amount), total * weights[0] // sum(weights)))
    least = 1 if total - largest >= amount - 1 else 0
    holding, rest = [largest] + [least] * (amount - 1), total - largest - least * (amount - 1)
    while rest > 0:
        movable = [i for i in range(1, amount) if holding[i] < largest] or [i for i in range(1, amount) if holding[i] < reach]
        whole, remaining = sum([weights[i] for i in movable]), rest
        for i in movable:
            extra = min(reach - holding[i], max(1, remaining * weights[i] // whole), rest)
            holding[i] = holding[i] + extra
            rest = rest - extra
    return np.array(holding)


def normal_values(rng, extent, deviation, reach, pieces=(), held_as=jnp.bfloat16):
    factor_of = block_levels(rng, extent, pieces, -0.22, 0.18) if pieces else 1.0
    drawn = jax.random.normal(rng, extent, jnp.float32) * deviation * factor_of
    return jnp.minimum(jnp.maximum(drawn, -reach), reach).astype(held_as)


def setup_inputs(seed: int = 0) -> dict:
    streams_of = jax.random.split(jax.random.key(seed), 6)
    master = normal_values(streams_of[0], (GROUPS, ROWS, COLS), 1.0, 6.0, ((0, 4), (1, 64)), jnp.float32)
    first_moment = normal_values(streams_of[1], (GROUPS, ROWS, COLS), 0.01, 0.06, ((0, 4), (1, 64)), jnp.float32)
    second_moment = jnp.clip(jnp.exp(math.log(0.001) - 4.6051703 * jax.random.uniform(streams_of[2], (GROUPS, ROWS, COLS), jnp.float32) ** block_levels(streams_of[2], (GROUPS, ROWS, COLS), ((0, 4), (1, 64)), -0.2, 0.2)), 9.999999747378752e-06, 0.001)
    rotation_keys = jax.random.split(jax.random.fold_in(streams_of[3], 1), ROUNDS * N_DP // N_DP)
    rotation_turns = jax.random.permutation(jax.random.fold_in(streams_of[3], 3), ROUNDS * N_DP // N_DP)
    rotation = jax.vmap(lambda own, number: shared_out(jax.random.fold_in(streams_of[3], 2), own, number, N_DP, N_DP, 1, MOST, 2))(rotation_keys, rotation_turns).reshape((ROUNDS, N_DP, 1))
    assignment = jax.random.permutation(streams_of[4], SPANS).astype(jnp.int32)
    return {"master": master, "first_moment": first_moment, "second_moment": second_moment, "rotation": rotation, "assignment": assignment}


BETA_ONE = 0.9
BETA_TWO = 0.95
EPSILON = 1e-08

def scaled_moment(first_part, second_part):
    corr_one = 1.0 - BETA_ONE ** STEP
    corr_two = 1.0 - BETA_TWO ** STEP
    return first_part / corr_one / (jnp.sqrt(second_part / corr_two) + EPSILON)

def slot_table(rotation, dp_count, most_slots):
    owners = rotation[:, :, 0]
    span_ids = jnp.arange(dp_count, dtype=jnp.int32)
    same_writer = owners[:, :, None] == owners[:, None, :]
    before = span_ids[None, :] < span_ids[:, None]
    slot_rank = lax.optimization_barrier(jnp.sum((same_writer & before[None]).astype(jnp.int32), axis=2))
    writers = jnp.arange(dp_count, dtype=jnp.int32)
    slot_ids = jnp.arange(most_slots, dtype=jnp.int32)
    matches = (owners[:, None, None, :] == writers[None, None, :, None]) & (slot_rank[:, None, None, :] == slot_ids[None, :, None, None])
    matches = matches.astype(jnp.int32)
    found_any = lax.optimization_barrier(jnp.sum(matches, axis=3))
    picked = lax.optimization_barrier(jnp.sum(matches * span_ids, axis=3))
    return (picked + (1 - found_any) * dp_count).astype(jnp.int32)

def position_weights(line_ids, per_row, lane_count):
    row_ids = line_ids // per_row
    col_ids = line_ids % per_row * lane_count
    lane_ids = jnp.arange(lane_count, dtype=jnp.int32)
    pattern = (row_ids[..., None] * 5 + (col_ids[..., None] + lane_ids) * 3) % 11
    return 1.0 + pattern.astype(jnp.float32) / 10.0

def reference(master, first_moment, second_moment, rotation, assignment):
    per_row = COLS // LANE
    lines_device = ROWS // N_DP * per_row
    piece_len = lines_device // (ROUNDS * N_DP)
    inv_count = 1.0 / math.sqrt(N_DP * piece_len * LANE)
    table = slot_table(rotation, N_DP, MOST)
    line_ids = jnp.arange(ROWS * per_row, dtype=jnp.int32).reshape(N_DP, ROUNDS, N_DP, piece_len)
    weights = position_weights(line_ids, per_row, LANE)
    round_ids = jnp.arange(ROUNDS, dtype=jnp.int32)[:, None, None]

    def arrange_field(field_in):
        line_view = field_in.reshape(N_DP, ROUNDS, N_DP, piece_len, LANE)
        totals = lax.optimization_barrier(jnp.sum(line_view * weights, axis=(0, 3, 4))) * inv_count
        reordered = jnp.transpose(line_view, (1, 2, 0, 3, 4))
        padded = jnp.concatenate([reordered, jnp.zeros((ROUNDS, 1, N_DP, piece_len, LANE), reordered.dtype)], axis=1)
        selected = padded[round_ids, table]
        saved_rows = jnp.transpose(selected, (2, 0, 1, 3, 4, 5)).reshape(N_DP * ROUNDS, MOST, N_DP * piece_len, LANE)
        return (saved_rows, totals.reshape(ROUNDS * N_DP))

    def one_group(fields):
        master_part, first_part, second_part = fields
        update = scaled_moment(first_part, second_part)
        saved_master, master_sums = arrange_field(master_part)
        saved_update, update_sums = arrange_field(update)
        return (saved_master, saved_update, jnp.stack([master_sums, update_sums]))
    saved_master, saved_update, group_sums = lax.map(one_group, (master, first_moment, second_moment))
    checksums = jnp.zeros_like(group_sums).at[:, :, assignment.astype(jnp.int32)].set(group_sums)
    return (saved_master, saved_update, checksums)
```

```python
import functools
import math

import jax
import jax.numpy as jnp
from jax import lax
from jax.experimental import pallas as pl
from jax.experimental.pallas import tpu as pltpu
from jax.sharding import Mesh
from jax.sharding import PartitionSpec as P

LANE = 128
MOST = 3
STEP = 20
BETA_ONE = 0.9
BETA_TWO = 0.95
EPSILON = 1e-08
DP = ("dp_0", "dp_1", "dp_2")
EXPERT = ("expert_0", "expert_1")
MESH = pl.DeviceIdType.MESH

N = 4
ROUNDS = 4
SPANS = 256
PIECE = 7
SLOTS = ROUNDS * MOST
BLOCK = N * SLOTS
PLANE = N * N
USUAL = 96
ALL = PLANE * SLOTS


def three_parts(x):
    hi = x.astype(jnp.bfloat16)
    rest = x - hi.astype(jnp.float32)
    mid = rest.astype(jnp.bfloat16)
    low = (rest - mid.astype(jnp.float32)).astype(jnp.bfloat16)
    return hi, mid, low


def select_rows(choice, x):
    hi, mid, low = (
        jnp.dot(choice, part, preferred_element_type=jnp.float32) for part in three_parts(x)
    )
    return hi + mid + low


def prepare(room, master, first, second, rot_row, rot_col, packed, sums, target, lin_m, lin_u):
    x, z, y = (lax.axis_index(axis) for axis in DP)
    position = (x * N + z) * N + y
    corr_one = 1.0 - BETA_ONE**STEP
    corr_two = 1.0 - BETA_TWO**STEP
    per_row = master.shape[1] // LANE
    rows = master.shape[0]
    for col in range(per_row):
        at = slice(col * LANE, (col + 1) * LANE)
        lin_m[pl.ds(col, rows, stride=per_row), :] = master[:, at]
        lin_u[pl.ds(col, rows, stride=per_row), :] = (first[:, at] / corr_one) / (
            jnp.sqrt(second[:, at] / corr_two) + EPSILON
        )

    row_id = lax.broadcasted_iota(jnp.int32, (SPANS, SPANS), 0)
    col_id = lax.broadcasted_iota(jnp.int32, (SPANS, SPANS), 1)
    w_row, w_col = rot_row[...], rot_col[...]
    z_row, z_col = (w_row // N) % N, (w_col // N) % N
    same_z = z_col == z_row
    place_row = jnp.sum(jnp.where(same_z & (row_id < col_id), 1, 0), axis=0, keepdims=True)
    place_col = jnp.sum(jnp.where(same_z & (col_id < row_id), 1, 0), axis=1, keepdims=True)
    same_w = (w_col == w_row) & (row_id // (N * PLANE) == col_id // (N * PLANE))
    slot_col = jnp.sum(jnp.where(same_w & (col_id < row_id), 1, 0), axis=1, keepdims=True)

    lines = lax.broadcasted_iota(jnp.int32, (N * room, SPANS), 0)
    choice = (lines == z_row * room + place_row).astype(jnp.float32).astype(jnp.bfloat16)

    round_col = lax.broadcasted_iota(jnp.int32, (SPANS, 1), 0) // (N * PLANE)
    writer_col = (w_col // PLANE) * N + w_col % N
    value_col = writer_col * (2 * SLOTS) + round_col * MOST + slot_col
    lane = lax.broadcasted_iota(jnp.int32, (SPANS, 2 * room), 1)
    second_half = lane >= room
    here = (z_col == z) & (place_col == jnp.where(second_half, lane - room, lane))
    value = value_col + jnp.where(second_half, SLOTS, 0)
    found = jnp.sum(jnp.where(here, value + 1, 0), axis=0, keepdims=True) - 1
    target[...] = jnp.broadcast_to(found, target.shape)

    total_m = jnp.zeros((SPANS, LANE), jnp.float32)
    total_u = jnp.zeros((SPANS, LANE), jnp.float32)
    span = lax.broadcasted_iota(jnp.int32, (SPANS, LANE), 0)
    entry = lax.broadcasted_iota(jnp.int32, (SPANS, LANE), 1)
    shift = (5 * rows * position) % 11
    for part in range(PIECE):
        x_m = lin_m[pl.ds(part, SPANS, stride=PIECE), :]
        x_u = lin_u[pl.ds(part, SPANS, stride=PIECE), :]
        line = span * PIECE + part
        number = 5 * (line // per_row) + 3 * ((line % per_row) * LANE + entry) + shift
        number = number.astype(jnp.float32)
        pattern = number - 11.0 * jnp.floor((number + 0.5) * (1.0 / 11.0))
        weight = 1.0 + pattern * 0.1
        total_m += x_m * weight
        total_u += x_u * weight
        packed[part] = select_rows(choice, jnp.concatenate([x_m, x_u], axis=1))

    scale = 1.0 / math.sqrt(N * PLANE * PIECE * LANE)
    ones = jnp.ones((8, LANE), jnp.float32)
    sums[...] = jnp.zeros_like(sums)
    for i, total in enumerate((total_m, total_u)):
        row = scale * lax.dot_general(
            ones,
            total,
            (((1,), (1,)), ((), ())),
            precision=lax.Precision.HIGHEST,
            preferred_element_type=jnp.float32,
        )
        for half in range(2):
            sums[2 * i + half : 2 * i + half + 1, :] = row[0:1, half * LANE : (half + 1) * LANE]


def exchange(
    room,
    packed,
    sums,
    target,
    out,
    sums_out,
    near,
    ready,
    sums_z,
    sums_p,
    sums_e,
    line_sum,
    plane_sum,
    own_sem,
    keep_sem,
    z_send,
    z_recv,
    p_send,
    p_recv,
    s_send,
    s_recv,
):
    x, z, y = (lax.axis_index(axis) for axis in DP)
    e_0, e_1 = (lax.axis_index(axis) for axis in EXPERT)
    here = x * N + y

    def on_line(step):
        return lax.rem(z + step, N)

    def in_plane(step):
        return lax.rem(x + step // N, N), lax.rem(y + step % N, N)

    def line_id(step):
        return {"dp_1": on_line(step)}

    def plane_id(step):
        to_x, to_y = in_plane(step)
        return {"dp_0": to_x, "dp_2": to_y}

    def expert_id(step):
        return {"expert_0": lax.rem(e_0 + step // 2, 2), "expert_1": lax.rem(e_1 + step % 2, 2)}

    barrier = pltpu.get_barrier_semaphore()
    others = [line_id(s) for s in range(1, N)]
    others += [plane_id(s) for s in range(1, PLANE)]
    others += [expert_id(s) for s in range(1, N)]
    for other in others:
        pl.semaphore_signal(barrier, inc=1, device_id=other, device_id_type=MESH)
    pl.semaphore_wait(barrier, len(others))

    def send(src, dst, send_sem, recv_sem, device):
        copy = pltpu.make_async_remote_copy(
            src_ref=src,
            dst_ref=dst,
            send_sem=send_sem,
            recv_sem=recv_sem,
            device_id=device,
            device_id_type=MESH,
        )
        copy.start()
        return copy

    sum_line = [
        send(sums, sums_z.at[z], s_send.at[s - 1], s_recv.at[s - 1], line_id(s))
        for s in range(1, N)
    ]
    sums_z[z] = sums[...]

    mine = pl.ds(pl.multiple_of(z * room, 8), room)
    lines = []
    for part in range(PIECE):
        for s in (2, 1, 3):
            theirs = pl.ds(pl.multiple_of(on_line(s) * room, 8), room)
            lines.append(
                send(
                    packed.at[part, theirs],
                    near.at[part, mine],
                    z_send.at[part, s - 1],
                    z_recv.at[part, s - 1],
                    line_id(s),
                )
            )
    owns = []
    for part in range(PIECE):
        own = pltpu.make_async_copy(packed.at[part, mine], near.at[part, mine], own_sem.at[part])
        own.start()
        owns.append(own)

    wide = lax.broadcasted_iota(jnp.int32, (2 * BLOCK // 4 * PLANE, 2 * room), 0)
    choice = (wide == target[0:1, :]).astype(jnp.float32).astype(jnp.bfloat16)
    home = pl.ds(pl.multiple_of(here * BLOCK, 8), BLOCK)
    planes, sum_plane, sum_expert = [], [], []
    for part in range(PIECE):
        owns[part].wait()
        for copy in lines[3 * part : 3 * part + 3]:
            copy.wait_recv()
        if part == 0:
            for copy in sum_line:
                copy.wait_recv()
            line_sum[...] = sums_z[0] + sums_z[1] + sums_z[2] + sums_z[3]
            sums_p[here] = line_sum[...]
            for s in range(1, PLANE):
                at = N - 2 + s
                sum_plane.append(
                    send(line_sum, sums_p.at[here], s_send.at[at], s_recv.at[at], plane_id(s))
                )
        if part == 2:
            for copy in sum_plane:
                copy.wait_recv()
            total = sums_p[0]
            for d in range(1, PLANE):
                total = total + sums_p[d]
            plane_sum[...] = total
            sums_e[e_0 * 2 + e_1] = total
            for s in range(1, N):
                at = N + PLANE - 3 + s
                sum_expert.append(
                    send(
                        plane_sum,
                        sums_e.at[e_0 * 2 + e_1],
                        s_send.at[at],
                        s_recv.at[at],
                        expert_id(s),
                    )
                )
        for half in range(2):
            got = select_rows(choice, near[part, 2 * room * half : 2 * room * (half + 1), :])
            rows = slice(2 * SLOTS * half, 2 * SLOTS * (half + 1))
            for t in range(2):
                ready[part, :, t, rows, :] = got[:, t * LANE : (t + 1) * LANE].reshape(
                    PLANE, 2 * SLOTS, LANE
                )
        for i in range(1, PLANE):
            s = 1 + (i - 1 + 2 * part) % (PLANE - 1)
            to_x, to_y = in_plane(s)
            planes.append(
                send(
                    ready.at[part, to_x * N + to_y],
                    out.at[part, :, home],
                    p_send.at[part, s - 1],
                    p_recv.at[part, s - 1],
                    plane_id(s),
                )
            )
        keep = pltpu.make_async_copy(ready.at[part, here], out.at[part, :, home], keep_sem.at[part])
        keep.start()
        owns.append(keep)

    for copy in sum_expert:
        copy.wait_recv()
    sums_out[...] = sums_e[...]
    for copy in owns[PIECE:]:
        copy.wait()
    for copy in lines + sum_line + sum_plane + sum_expert:
        copy.wait_send()
    for copy in planes:
        copy.wait()


def unpack(got, sums, file_slot, saved_m, saved_u, checks, lines, full_m, full_u, both, in_sem, out_sem):
    copies = []
    for part in range(PIECE):
        copy = pltpu.make_async_copy(got.at[part], lines.at[part], in_sem.at[part])
        copy.start()
        copies.append(copy)

    for g in range(N):
        for i in range(2):
            for half in range(2):
                both[2 * g + i : 2 * g + i + 1, half * LANE : (half + 1) * LANE] = sums[
                    g, 2 * i + half : 2 * i + half + 1, :
                ]
    lane = lax.broadcasted_iota(jnp.int32, (SPANS, SPANS), 1)
    placing = (file_slot[...] == lane).astype(jnp.float32)
    checks[...] = jnp.dot(
        both[...],
        placing,
        precision=lax.Precision.HIGHEST,
        preferred_element_type=jnp.float32,
    )

    for part in range(PIECE):
        copies[part].wait()

        def one_slot(slot, _, part=part):
            for t, full in enumerate((full_m, full_u)):
                for to_x in range(N):
                    for to_z in range(N):
                        rows = lines[
                            part, t, pl.ds(to_x * N * BLOCK + to_z * SLOTS + slot, N, stride=BLOCK), :
                        ]
                        first = (to_x * PLANE + to_z * N) * PIECE + part
                        full[slot, pl.ds(first, N, stride=PIECE), :] = rows
            return _

        lax.fori_loop(0, SLOTS, one_slot, 0)
    outs = [
        pltpu.make_async_copy(full_m, saved_m, out_sem.at[0]),
        pltpu.make_async_copy(full_u, saved_u, out_sem.at[1]),
    ]
    for copy in outs:
        copy.start()
    for copy in outs:
        copy.wait()


VMEM = pl.BlockSpec(memory_space=pltpu.VMEM)
ANY = pl.BlockSpec(memory_space=pl.ANY)
F32 = jnp.float32


def move(room, number, master, first, second, rot_row, rot_col):
    lines = master.shape[0] * master.shape[1] // LANE
    packed, sums, target = pl.pallas_call(
        functools.partial(prepare, room),
        out_shape=(
            jax.ShapeDtypeStruct((PIECE, N * room, 2 * LANE), F32),
            jax.ShapeDtypeStruct((8, LANE), F32),
            jax.ShapeDtypeStruct((8, 2 * room), jnp.int32),
        ),
        in_specs=[VMEM] * 5,
        out_specs=(VMEM, VMEM, VMEM),
        scratch_shapes=[pltpu.VMEM((lines, LANE), F32), pltpu.VMEM((lines, LANE), F32)],
    )(master, first, second, rot_row, rot_col)
    small = 2 * (N - 1) + PLANE - 1
    return pl.pallas_call(
        functools.partial(exchange, room),
        out_shape=(
            jax.ShapeDtypeStruct((PIECE, 2, PLANE * BLOCK, LANE), F32),
            jax.ShapeDtypeStruct((N, 8, LANE), F32),
        ),
        in_specs=[VMEM] * 3,
        out_specs=(ANY, VMEM),
        scratch_shapes=[
            pltpu.VMEM((PIECE, N * room, 2 * LANE), F32),
            pltpu.VMEM((PIECE, PLANE, 2, BLOCK, LANE), F32),
            pltpu.VMEM((N, 8, LANE), F32),
            pltpu.VMEM((PLANE, 8, LANE), F32),
            pltpu.VMEM((N, 8, LANE), F32),
            pltpu.VMEM((8, LANE), F32),
            pltpu.VMEM((8, LANE), F32),
            pltpu.SemaphoreType.DMA((PIECE,)),
            pltpu.SemaphoreType.DMA((PIECE,)),
            pltpu.SemaphoreType.DMA((PIECE, N - 1)),
            pltpu.SemaphoreType.DMA((PIECE, N - 1)),
            pltpu.SemaphoreType.DMA((PIECE, PLANE - 1)),
            pltpu.SemaphoreType.DMA((PIECE, PLANE - 1)),
            pltpu.SemaphoreType.DMA((small,)),
            pltpu.SemaphoreType.DMA((small,)),
        ],
        compiler_params=pltpu.CompilerParams(collective_id=number, has_side_effects=True),
    )(packed, sums, target)


def shards(master, first, second, rotation, assignment):
    owners = rotation.reshape(1, SPANS)
    planes = jnp.arange(N, dtype=jnp.int32)[:, None]
    load = jnp.sum(((owners // N) % N == planes).astype(jnp.int32), axis=1)
    got, sums = lax.cond(
        jnp.max(load) <= USUAL,
        functools.partial(move, USUAL, 0),
        functools.partial(move, ALL, 1),
        master[0],
        first[0],
        second[0],
        owners,
        rotation.reshape(SPANS, 1),
    )
    length = N * PLANE * PIECE
    saved_m, saved_u, checks = pl.pallas_call(
        unpack,
        out_shape=(
            jax.ShapeDtypeStruct((SLOTS, length, LANE), F32),
            jax.ShapeDtypeStruct((SLOTS, length, LANE), F32),
            jax.ShapeDtypeStruct((2 * N, SPANS), F32),
        ),
        in_specs=[ANY, VMEM, VMEM],
        out_specs=(ANY, ANY, VMEM),
        scratch_shapes=[
            pltpu.VMEM((PIECE, 2, PLANE * BLOCK, LANE), F32),
            pltpu.VMEM((SLOTS, length, LANE), F32),
            pltpu.VMEM((SLOTS, length, LANE), F32),
            pltpu.VMEM((2 * N, SPANS), F32),
            pltpu.SemaphoreType.DMA((PIECE,)),
            pltpu.SemaphoreType.DMA((2,)),
        ],
    )(got, sums, assignment.reshape(SPANS, 1))
    shape = (1, ROUNDS, MOST, length, LANE)
    return saved_m.reshape(shape), saved_u.reshape(shape), checks.reshape(N, 2, SPANS)


def solution(mesh):
    torus = Mesh(mesh.devices.reshape(N, N, N, 2, 2), DP + EXPERT)
    rows = P(EXPERT, DP, None)
    saved = P(EXPERT, DP, None, None, None)
    return jax.shard_map(
        shards,
        mesh=torus,
        in_specs=(rows, rows, rows, P(), P()),
        out_specs=(saved, saved, P()),
        check_vma=False,
    )
```

```python
import functools
import math

import jax
import jax.numpy as jnp
from jax import lax
from jax.experimental import pallas as pl
from jax.experimental.pallas import tpu as pltpu
from jax.sharding import Mesh
from jax.sharding import PartitionSpec as P

LANE = 128
MOST = 3
STEP = 20
BETA_ONE = 0.9
BETA_TWO = 0.95
EPSILON = 1e-08
DP = ("dp_0", "dp_1", "dp_2")
EXPERT = ("expert_0", "expert_1")
MESH = pl.DeviceIdType.MESH

N = 4
ROUNDS = 4
SPANS = 256
PIECE = 7
SLOTS = ROUNDS * MOST
BLOCK = N * SLOTS
PLANE = N * N
USUAL = 96
PARTS = 2 * PIECE
AHEAD = 2
ALL = PLANE * SLOTS


def three_parts(x):
    hi = x.astype(jnp.bfloat16)
    rest = x - hi.astype(jnp.float32)
    mid = rest.astype(jnp.bfloat16)
    low = (rest - mid.astype(jnp.float32)).astype(jnp.bfloat16)
    return hi, mid, low


def select_rows(choice, x):
    parts = jnp.concatenate(three_parts(x), axis=1)
    got = jnp.dot(choice, parts, preferred_element_type=jnp.float32)
    width = x.shape[1]
    return got[:, :width] + got[:, width : 2 * width] + got[:, 2 * width :]


def flat_row(rotation, flat):
    width = rotation.shape[1]
    for r in range(ROUNDS):
        flat[0:1, r * width : (r + 1) * width] = rotation[r : r + 1, :]
    return flat[0:1, :]


def plane_load(rotation, fits):
    plane = (rotation[...] // N) % N
    load = [jnp.sum(jnp.where(plane == k, 1.0, 0.0)) for k in range(N)]
    most = functools.reduce(jnp.maximum, load)
    fits[0] = (most <= USUAL).astype(jnp.int32)


def exchange(
    room,
    master,
    first,
    second,
    rotation,
    out,
    sums_out,
    in_m,
    in_one,
    in_two,
    flat,
    lin_m,
    lin_u,
    packed,
    near,
    ready,
    sums,
    sums_z,
    sums_p,
    sums_e,
    line_sum,
    plane_sum,
    in_sem,
    own_sem,
    keep_sem,
    z_send,
    z_recv,
    p_send,
    p_recv,
    s_send,
    s_recv,
):
    x, z, y = (lax.axis_index(axis) for axis in DP)
    e_0, e_1 = (lax.axis_index(axis) for axis in EXPERT)
    here = x * N + y

    loads = []
    for i, (src, dst) in enumerate(((master, in_m), (first, in_one), (second, in_two))):
        load = pltpu.make_async_copy(src, dst, in_sem.at[i])
        load.start()
        loads.append(load)

    def on_line(step):
        return lax.rem(z + step, N)

    def in_plane(step):
        return lax.rem(x + step // N, N), lax.rem(y + step % N, N)

    def line_id(step):
        return {"dp_1": on_line(step)}

    def plane_id(step):
        to_x, to_y = in_plane(step)
        return {"dp_0": to_x, "dp_2": to_y}

    def expert_id(step):
        return {"expert_0": lax.rem(e_0 + step // 2, 2), "expert_1": lax.rem(e_1 + step % 2, 2)}

    barrier = pltpu.get_barrier_semaphore()
    others = [line_id(s) for s in range(1, N)]
    others += [plane_id(s) for s in range(1, PLANE)]
    others += [expert_id(s) for s in range(1, N)]
    for other in others:
        pl.semaphore_signal(barrier, inc=1, device_id=other, device_id_type=MESH)

    def send(src, dst, send_sem, recv_sem, device):
        copy = pltpu.make_async_remote_copy(
            src_ref=src,
            dst_ref=dst,
            send_sem=send_sem,
            recv_sem=recv_sem,
            device_id=device,
            device_id_type=MESH,
        )
        copy.start()
        return copy

    row_id = lax.broadcasted_iota(jnp.int32, (SPANS, SPANS), 0)
    col_id = lax.broadcasted_iota(jnp.int32, (SPANS, SPANS), 1)
    w_row = flat_row(rotation, flat)
    w_col = jnp.sum(jnp.where(row_id == col_id, w_row, 0), axis=1, keepdims=True)
    z_row, z_col = (w_row // N) % N, (w_col // N) % N
    same_z = z_col == z_row
    place_row = jnp.sum(jnp.where(same_z & (row_id < col_id), 1, 0), axis=0, keepdims=True)
    lines_id = lax.broadcasted_iota(jnp.int32, (N * room, SPANS), 0)
    by_plane = (lines_id == z_row * room + place_row).astype(jnp.float32).astype(jnp.bfloat16)

    rows, per_row = in_m.shape[0], in_m.shape[1] // LANE
    loads[0].wait()
    for col in range(per_row):
        at = slice(col * LANE, (col + 1) * LANE)
        lin_m[pl.ds(col, rows, stride=per_row), :] = in_m[:, at]

    def piece_lines(part):
        source = (lin_m, lin_u)[part // PIECE]
        return source[pl.ds(part % PIECE, SPANS, stride=PIECE), :]

    mine = pl.ds(pl.multiple_of(z * room, 8), room)
    lines, owns = [], []

    def pack(part):
        packed[part] = select_rows(by_plane, piece_lines(part))

    def send_line(part):
        for s in (2, 1, 3):
            theirs = pl.ds(pl.multiple_of(on_line(s) * room, 8), room)
            lines.append(
                send(
                    packed.at[part, theirs],
                    near.at[part, mine],
                    z_send.at[part, s - 1],
                    z_recv.at[part, s - 1],
                    line_id(s),
                )
            )
        own = pltpu.make_async_copy(packed.at[part, mine], near.at[part, mine], own_sem.at[part])
        own.start()
        owns.append(own)

    pack(0)
    pl.semaphore_wait(barrier, len(others))
    send_line(0)
    for part in range(1, AHEAD):
        pack(part)
        send_line(part)

    corr_one = 1.0 - BETA_ONE**STEP
    corr_two = 1.0 - BETA_TWO**STEP
    loads[1].wait()
    loads[2].wait()
    for col in range(per_row):
        at = slice(col * LANE, (col + 1) * LANE)
        lin_u[pl.ds(col, rows, stride=per_row), :] = (in_one[:, at] / corr_one) / (
            jnp.sqrt(in_two[:, at] / corr_two) + EPSILON
        )
    totals = [jnp.zeros((SPANS, LANE), jnp.float32) for _ in range(2)]
    span = lax.broadcasted_iota(jnp.int32, (SPANS, LANE), 0)
    entry = lax.broadcasted_iota(jnp.int32, (SPANS, LANE), 1)
    shift = (5 * rows * ((x * N + z) * N + y)) % 11
    for part in range(PIECE):
        line = span * PIECE + part
        number = 5 * (line // per_row) + 3 * ((line % per_row) * LANE + entry) + shift
        number = number.astype(jnp.float32)
        pattern = number - 11.0 * jnp.floor((number + 0.5) * (1.0 / 11.0))
        weight = 1.0 + pattern * 0.1
        for t in range(2):
            totals[t] += piece_lines(t * PIECE + part) * weight
    scale = 1.0 / math.sqrt(N * PLANE * PIECE * LANE)
    ones = jnp.ones((8, LANE), jnp.float32)
    sums[...] = jnp.zeros_like(sums)
    for t in range(2):
        row = scale * lax.dot_general(
            ones,
            totals[t],
            (((1,), (1,)), ((), ())),
            precision=lax.Precision.HIGHEST,
            preferred_element_type=jnp.float32,
        )
        for half in range(2):
            sums[2 * t + half : 2 * t + half + 1, :] = row[0:1, half * LANE : (half + 1) * LANE]
    sums_z[z] = sums[...]
    sum_line = [
        send(sums, sums_z.at[z], s_send.at[s - 1], s_recv.at[s - 1], line_id(s))
        for s in range(1, N)
    ]

    place_col = jnp.sum(jnp.where(same_z & (col_id < row_id), 1, 0), axis=1, keepdims=True)
    same_w = (w_col == w_row) & (row_id // (N * PLANE) == col_id // (N * PLANE))
    slot_col = jnp.sum(jnp.where(same_w & (col_id < row_id), 1, 0), axis=1, keepdims=True)
    round_col = lax.broadcasted_iota(jnp.int32, (SPANS, 1), 0) // (N * PLANE)
    writer_col = (w_col // PLANE) * N + w_col % N
    value_col = writer_col * (2 * SLOTS) + round_col * MOST + slot_col
    lane = lax.broadcasted_iota(jnp.int32, (SPANS, 2 * room), 1)
    second_half = lane >= room
    found = (z_col == z) & (place_col == jnp.where(second_half, lane - room, lane))
    value = value_col + jnp.where(second_half, SLOTS, 0)
    target = jnp.sum(jnp.where(found, value + 1, 0), axis=0, keepdims=True) - 1
    wide = lax.broadcasted_iota(jnp.int32, (2 * SLOTS * PLANE, 2 * room), 0)
    by_writer = (wide == target).astype(jnp.float32).astype(jnp.bfloat16)

    home = pl.ds(pl.multiple_of((y * N + x) * BLOCK, 8), BLOCK)
    planes, keeps, sum_plane, sum_expert = [], [], [], []
    for part in range(PARTS):
        if part + AHEAD < PARTS:
            pack(part + AHEAD)
        for copy in lines[3 * part : 3 * part + 3]:
            copy.wait_recv()
        if part + AHEAD < PARTS:
            send_line(part + AHEAD)
        owns[part].wait()
        if part == 1:
            for copy in sum_line:
                copy.wait_recv()
            line_sum[...] = sums_z[0] + sums_z[1] + sums_z[2] + sums_z[3]
            sums_p[here] = line_sum[...]
            for s in range(1, PLANE):
                at = N - 2 + s
                sum_plane.append(
                    send(line_sum, sums_p.at[here], s_send.at[at], s_recv.at[at], plane_id(s))
                )
        if part == 6:
            for copy in sum_plane:
                copy.wait_recv()
            total = sums_p[0]
            for d in range(1, PLANE):
                total = total + sums_p[d]
            plane_sum[...] = total
            sums_e[e_0 * 2 + e_1] = total
            for s in range(1, N):
                at = N + PLANE - 3 + s
                sum_expert.append(
                    send(
                        plane_sum,
                        sums_e.at[e_0 * 2 + e_1],
                        s_send.at[at],
                        s_recv.at[at],
                        expert_id(s),
                    )
                )
        for half in range(2):
            got = select_rows(by_writer, near[part, 2 * room * half : 2 * room * (half + 1), :])
            at = slice(2 * SLOTS * half, 2 * SLOTS * (half + 1))
            ready[part, :, at, :] = got.reshape(PLANE, 2 * SLOTS, LANE)
        for i in range(PLANE - 1):
            s = 1 + (i + 4 * part) % (PLANE - 1)
            to_x, to_y = in_plane(s)
            planes.append(
                send(
                    ready.at[part, to_x * N + to_y],
                    out.at[part, home],
                    p_send.at[part, s - 1],
                    p_recv.at[part, s - 1],
                    plane_id(s),
                )
            )
        keep = pltpu.make_async_copy(ready.at[part, here], out.at[part, home], keep_sem.at[part])
        keep.start()
        keeps.append(keep)

    for copy in sum_expert:
        copy.wait_recv()
    sums_out[...] = sums_e[...]
    for copy in keeps:
        copy.wait()
    for copy in lines + sum_line + sum_plane + sum_expert:
        copy.wait_send()
    for copy in planes:
        copy.wait()


def unpack(got, sums, file_slot, saved_m, saved_u, checks, lines, full_m, full_u, both, in_sem, out_sem):
    copies = []
    for part in range(PARTS):
        copy = pltpu.make_async_copy(got.at[part], lines.at[part], in_sem.at[part])
        copy.start()
        copies.append(copy)

    for g in range(N):
        for i in range(2):
            for half in range(2):
                both[2 * g + i : 2 * g + i + 1, half * LANE : (half + 1) * LANE] = sums[
                    g, 2 * i + half : 2 * i + half + 1, :
                ]
    slot_id = lax.broadcasted_iota(jnp.int32, (SPANS, SPANS), 0)
    placing = (file_slot[...] == slot_id).astype(jnp.float32)
    placed = lax.dot_general(
        both[...],
        placing,
        (((1,), (1,)), ((), ())),
        precision=lax.Precision.HIGHEST,
        preferred_element_type=jnp.float32,
    )
    for g in range(N):
        checks[g] = placed[2 * g : 2 * g + 2, :]

    def move_lines(part, slot, full):
        for at_y in range(N):
            rows = lines[part, pl.ds(at_y * N * BLOCK + slot, PLANE, stride=SLOTS), :]
            full[slot, pl.ds(at_y * PIECE + part % PIECE, PLANE, stride=N * PIECE), :] = rows

    outs = []
    for part in range(PIECE):
        copies[part].wait()
        for slot in range(SLOTS):
            move_lines(part, slot, full_m)
    copy = pltpu.make_async_copy(full_m, saved_m, out_sem.at[SLOTS])
    copy.start()
    outs.append(copy)
    for part in range(PIECE, PARTS):
        copies[part].wait()
    for slot in range(SLOTS):
        for part in range(PIECE, PARTS):
            move_lines(part, slot, full_u)
        copy = pltpu.make_async_copy(full_u.at[slot], saved_u.at[slot], out_sem.at[slot])
        copy.start()
        outs.append(copy)
    for copy in outs:
        copy.wait()


SMEM = pl.BlockSpec(memory_space=pltpu.SMEM)
VMEM = pl.BlockSpec(memory_space=pltpu.VMEM)
ANY = pl.BlockSpec(memory_space=pl.ANY)
F32 = jnp.float32


def move(room, number, master, first, second, rotation):
    rows, cols = master.shape
    lines = rows * cols // LANE
    small = 2 * (N - 1) + PLANE - 1
    return pl.pallas_call(
        functools.partial(exchange, room),
        out_shape=(
            jax.ShapeDtypeStruct((PARTS, PLANE * BLOCK, LANE), F32),
            jax.ShapeDtypeStruct((N, 8, LANE), F32),
        ),
        in_specs=[ANY, ANY, ANY, VMEM],
        out_specs=(ANY, VMEM),
        scratch_shapes=[
            pltpu.VMEM((rows, cols), F32),
            pltpu.VMEM((rows, cols), F32),
            pltpu.VMEM((rows, cols), F32),
            pltpu.VMEM((8, SPANS), jnp.int32),
            pltpu.VMEM((lines, LANE), F32),
            pltpu.VMEM((lines, LANE), F32),
            pltpu.VMEM((PARTS, N * room, LANE), F32),
            pltpu.VMEM((PARTS, N * room, LANE), F32),
            pltpu.VMEM((PARTS, PLANE, BLOCK, LANE), F32),
            pltpu.VMEM((8, LANE), F32),
            pltpu.VMEM((N, 8, LANE), F32),
            pltpu.VMEM((PLANE, 8, LANE), F32),
            pltpu.VMEM((N, 8, LANE), F32),
            pltpu.VMEM((8, LANE), F32),
            pltpu.VMEM((8, LANE), F32),
            pltpu.SemaphoreType.DMA((3,)),
            pltpu.SemaphoreType.DMA((PARTS,)),
            pltpu.SemaphoreType.DMA((PARTS,)),
            pltpu.SemaphoreType.DMA((PARTS, N - 1)),
            pltpu.SemaphoreType.DMA((PARTS, N - 1)),
            pltpu.SemaphoreType.DMA((PARTS, PLANE - 1)),
            pltpu.SemaphoreType.DMA((PARTS, PLANE - 1)),
            pltpu.SemaphoreType.DMA((small,)),
            pltpu.SemaphoreType.DMA((small,)),
        ],
        compiler_params=pltpu.CompilerParams(collective_id=number, has_side_effects=True),
    )(master, first, second, rotation)


def shards(master, first, second, rotation, assignment):
    rotation = rotation.reshape(ROUNDS, N * PLANE)
    fits = pl.pallas_call(
        plane_load,
        out_shape=jax.ShapeDtypeStruct((1,), jnp.int32),
        in_specs=[VMEM],
        out_specs=SMEM,
    )(rotation)
    got, sums = lax.cond(
        fits[0] > 0,
        functools.partial(move, USUAL, 0),
        functools.partial(move, ALL, 1),
        master[0],
        first[0],
        second[0],
        rotation,
    )
    length = N * PLANE * PIECE
    saved_m, saved_u, checks = pl.pallas_call(
        unpack,
        out_shape=(
            jax.ShapeDtypeStruct((SLOTS, length, LANE), F32),
            jax.ShapeDtypeStruct((SLOTS, length, LANE), F32),
            jax.ShapeDtypeStruct((N, 2, SPANS), F32),
        ),
        in_specs=[ANY, VMEM, VMEM],
        out_specs=(ANY, ANY, VMEM),
        scratch_shapes=[
            pltpu.VMEM((PARTS, PLANE * BLOCK, LANE), F32),
            pltpu.VMEM((SLOTS, length, LANE), F32),
            pltpu.VMEM((SLOTS, length, LANE), F32),
            pltpu.VMEM((2 * N, SPANS), F32),
            pltpu.SemaphoreType.DMA((PARTS,)),
            pltpu.SemaphoreType.DMA((SLOTS + 1,)),
        ],
    )(got, sums, assignment.reshape(1, SPANS))
    shape = (1, ROUNDS, MOST, length, LANE)
    return saved_m.reshape(shape), saved_u.reshape(shape), checks


def solution(mesh):
    torus = Mesh(mesh.devices.reshape(N, N, N, 2, 2), DP + EXPERT)
    rows = P(EXPERT, DP, None)
    saved = P(EXPERT, DP, None, None, None)
    return jax.shard_map(
        shards,
        mesh=torus,
        in_specs=(rows, rows, rows, P(), P()),
        out_specs=(saved, saved, P()),
        check_vma=False,
    )
```

```python
import functools
import math

import jax
import jax.numpy as jnp
from jax import lax
from jax.experimental import pallas as pl
from jax.experimental.pallas import tpu as pltpu
from jax.sharding import Mesh
from jax.sharding import PartitionSpec as P

LANE = 128
MOST = 3
STEP = 20
BETA_ONE = 0.9
BETA_TWO = 0.95
EPSILON = 1e-08
DP = ("dp_0", "dp_1", "dp_2")
EXPERT = ("expert_0", "expert_1")
MESH = pl.DeviceIdType.MESH

N = 4
ROUNDS = 4
SPANS = 256
PIECE = 7
PARTS = 2 * PIECE
SLOTS = ROUNDS * MOST
PLANE = N * N
BLOCK = PLANE * SLOTS
ROOMS = ((80, 32), (96, 40), (PLANE * SLOTS, N * SLOTS))
AHEAD = 2
LAG = 2


def three_parts(x):
    hi = x.astype(jnp.bfloat16)
    rest = x - hi.astype(jnp.float32)
    mid = rest.astype(jnp.bfloat16)
    low = (rest - mid.astype(jnp.float32)).astype(jnp.bfloat16)
    return hi, mid, low


def select_rows(choice, x):
    parts = jnp.concatenate(three_parts(x), axis=1)
    got = jnp.dot(choice, parts, preferred_element_type=jnp.float32)
    width = x.shape[1]
    return got[:, :width] + got[:, width : 2 * width] + got[:, 2 * width :]


def flat_row(rotation, flat):
    width = rotation.shape[1]
    for r in range(ROUNDS):
        flat[0:1, r * width : (r + 1) * width] = rotation[r : r + 1, :]
    return flat[0:1, :]


def which_room(rotation, choice, flat):
    w = flat_row(rotation, flat)
    x, z, y = w >> 4, (w >> 2) & 3, w & 3
    group = lax.broadcasted_iota(jnp.int32, (PLANE, SPANS), 0)
    in_plane, in_x, in_y = (
        jnp.max(jnp.sum(jnp.where(group == code, 1.0, 0.0), axis=1, keepdims=True))
        for code in (z, z * N + x, z * N + y)
    )
    in_line = jnp.maximum(in_x, in_y)
    misses = [((in_plane > room) | (in_line > line)) for room, line in ROOMS[:-1]]
    choice[0] = sum(miss.astype(jnp.int32) for miss in misses)


def exchange(
    room,
    line_room,
    master,
    first,
    second,
    rotation,
    out,
    sums_out,
    in_m,
    in_one,
    in_two,
    flat,
    flat_lines,
    packed,
    near,
    turned,
    close,
    ready,
    sums,
    part_sum,
    in_sem,
    own_sem,
    send_sem,
    recv_sem,
    s_send,
    s_recv,
):
    x, z, y = (lax.axis_index(axis) for axis in DP)
    e_0, e_1 = (lax.axis_index(axis) for axis in EXPERT)

    loads = []
    for i, (src, dst) in enumerate(((master, in_m), (first, in_one), (second, in_two))):
        load = pltpu.make_async_copy(src, dst, in_sem.at[i])
        load.start()
        loads.append(load)

    def step_from(place, step):
        return lax.rem(place + step, N)

    def z_peer(s):
        return {"dp_1": step_from(z, s)}

    def x_peer(s):
        return {"dp_0": step_from(x, s)}

    def y_peer(s):
        return {"dp_2": step_from(y, s)}

    def expert_peer(s):
        return {"expert_0": lax.rem(e_0 + s // 2, 2), "expert_1": lax.rem(e_1 + s % 2, 2)}

    hops = ((z, z_peer), (x, x_peer), (y, y_peer), (e_0 * 2 + e_1, expert_peer))
    barrier = pltpu.get_barrier_semaphore()
    for _, peer in hops:
        for s in range(1, N):
            pl.semaphore_signal(barrier, inc=1, device_id=peer(s), device_id_type=MESH)

    def to_peers(peer, src, dst, send_sems, recv_sems):
        return [
            pltpu.make_async_remote_copy(
                src_ref=src(s),
                dst_ref=dst,
                send_sem=send_sems.at[s - 1],
                recv_sem=recv_sems.at[s - 1],
                device_id=peer(s),
                device_id_type=MESH,
            )
            for s in (1, 3, 2)
        ]

    def start(*groups):
        for turn in range(N):
            for group in groups:
                group[turn].start()

    def arrived(copies):
        for copy in copies[:-1]:
            copy.wait_recv()
        copies[-1].wait()

    row_id = lax.broadcasted_iota(jnp.int32, (SPANS, SPANS), 0)
    col_id = lax.broadcasted_iota(jnp.int32, (SPANS, SPANS), 1)
    w_row = flat_row(rotation, flat)
    w_col = jnp.sum(jnp.where(row_id == col_id, w_row, 0), axis=1, keepdims=True)
    x_col, z_col, y_col = w_col >> 4, (w_col >> 2) & 3, w_col & 3
    x_row, z_row, y_row = w_row >> 4, (w_row >> 2) & 3, w_row & 3
    same_z = z_col == z_row
    place_row = jnp.sum(jnp.where(same_z & (row_id < col_id), 1, 0), axis=0, keepdims=True)

    def one_hot(count, target):
        ids = lax.broadcasted_iota(jnp.int32, (count, target.shape[1]), 0)
        return (ids == target).astype(jnp.float32).astype(jnp.bfloat16)

    by_plane = one_hot(N * room, z_row * room + place_row)

    rows, per_row = in_m.shape[0], in_m.shape[1] // LANE
    loads[0].wait()
    for col in range(per_row):
        at = slice(col * LANE, (col + 1) * LANE)
        flat_lines[pl.ds(col, rows, stride=per_row), :] = in_m[:, at]

    def piece_lines(part):
        first_line = part + (part // PIECE) * (rows * per_row - PIECE)
        return flat_lines[pl.ds(first_line, SPANS, stride=PIECE), :]

    def pack(part):
        got = select_rows(by_plane, piece_lines(part))
        packed[part] = got.reshape(N, room, LANE)

    def first_peers(part):
        return to_peers(
            z_peer,
            lambda s: packed.at[part, step_from(z, s)],
            near.at[part, z],
            send_sem.at[0, part],
            recv_sem.at[0, part],
        )

    def first_hop(part):
        own = pltpu.make_async_copy(packed.at[part, z], near.at[part, z], own_sem.at[0, part])
        return first_peers(part) + [own]

    pack(0)
    pl.semaphore_wait(barrier, len(hops) * (N - 1))
    start(first_hop(0))
    for part in range(1, AHEAD):
        pack(part)
        start(first_hop(part))

    corr_one = 1.0 - BETA_ONE**STEP
    corr_two = 1.0 - BETA_TWO**STEP
    loads[1].wait()
    loads[2].wait()
    for col in range(per_row):
        at = slice(col * LANE, (col + 1) * LANE)
        flat_lines[pl.ds(rows * per_row + col, rows, stride=per_row), :] = (in_one[:, at] / corr_one) / (
            jnp.sqrt(in_two[:, at] / corr_two) + EPSILON
        )
    totals = [jnp.zeros((SPANS, LANE), jnp.float32) for _ in range(2)]
    span = lax.broadcasted_iota(jnp.int32, (SPANS, LANE), 0)
    entry = lax.broadcasted_iota(jnp.int32, (SPANS, LANE), 1)
    shift = (5 * rows * ((x * N + z) * N + y)) % 11
    for part in range(PIECE):
        line = span * PIECE + part
        number = 5 * (line // per_row) + 3 * ((line % per_row) * LANE + entry) + shift
        number = number.astype(jnp.float32)
        pattern = number - 11.0 * jnp.floor((number + 0.5) * (1.0 / 11.0))
        weight = 1.0 + pattern * 0.1
        for t in range(2):
            totals[t] += piece_lines(t * PIECE + part) * weight
    scale = 1.0 / math.sqrt(N * PLANE * PIECE * LANE)
    ones = jnp.ones((8, LANE), jnp.float32)
    part_sum[0] = jnp.zeros((8, LANE), jnp.float32)
    for t in range(2):
        row = scale * lax.dot_general(
            ones,
            totals[t],
            (((1,), (1,)), ((), ())),
            precision=lax.Precision.HIGHEST,
            preferred_element_type=jnp.float32,
        )
        for half in range(2):
            part_sum[0, 2 * t + half : 2 * t + half + 1, :] = row[
                0:1, half * LANE : (half + 1) * LANE
            ]

    def sum_hop(hop):
        place, peer = hops[hop]
        return to_peers(
            peer,
            lambda s: part_sum.at[hop],
            sums.at[hop, place],
            s_send.at[hop],
            s_recv.at[hop],
        )

    def send_sums(hop):
        sums[hop, hops[hop][0]] = part_sum[hop]
        for copy in sum_hop(hop):
            copy.start()

    def add_sums(hop):
        for copy in sum_hop(hop):
            copy.wait_recv()
        part_sum[hop + 1] = sums[hop, 0] + sums[hop, 1] + sums[hop, 2] + sums[hop, 3]

    send_sums(0)

    before = col_id < row_id

    def count(same):
        return jnp.sum(jnp.where(same & before, 1, 0), axis=1, keepdims=True)

    place_col = count(same_z)
    in_round = (row_id >> 6) == (col_id >> 6)
    slot_col = count((w_col == w_row) & in_round)
    slot_col += (lax.broadcasted_iota(jnp.int32, (SPANS, 1), 0) >> 6) * MOST

    def found(at, value):
        return jnp.sum(jnp.where(at, value + 1, 0), axis=0, keepdims=True) - 1

    in_plane = z_col == z
    plane_at = lax.broadcasted_iota(jnp.int32, (1, room), 1)
    line_at = lax.broadcasted_iota(jnp.int32, (1, 2 * N * line_room), 1)
    source = jnp.zeros_like(line_at)
    for k in range(1, 2 * N):
        source += jnp.where(line_at >= k * line_room, 1, 0)
    line_at = line_at - source * line_room
    second_choice, last_choice = [], []
    for line_col, line_row, own, end_col in (
        (x_col, x_row, x, y_col),
        (y_col, y_row, y, x_col),
    ):
        in_line = count(same_z & (line_col == line_row))
        target = found(in_plane & (place_col == plane_at), line_col * line_room + in_line)
        second_choice.append(one_hot(N * line_room, target))
        here = in_plane & (line_col == own) & (in_line == line_at)
        target = found(here, end_col * (2 * N * SLOTS) + slot_col)
        target += jnp.where(target >= 0, source * SLOTS, 0)
        last_choice.append(one_hot(2 * N * N * SLOTS, target))

    def second_to(part, way):
        place = hops[1 + way][0]
        return close.at[part, place] if way == 0 else close.at[part, :, place]

    def second_peers(part, way):
        place, peer = hops[1 + way]
        return to_peers(
            peer,
            lambda s: turned.at[part, step_from(place, s)],
            second_to(part, way),
            send_sem.at[1, part],
            recv_sem.at[1, part],
        )

    def second_hop(part, way):
        own = pltpu.make_async_copy(
            turned.at[part, hops[1 + way][0]], second_to(part, way), own_sem.at[1, part]
        )
        return second_peers(part, way) + [own]

    def last_to(part, way):
        place = hops[2 - way][0]
        return out.at[part, pl.ds(pl.multiple_of(place * BLOCK, 8), BLOCK)]

    def last_peers(part, way):
        place, peer = hops[2 - way]
        return to_peers(
            peer,
            lambda s: ready.at[part, step_from(place, s)],
            last_to(part, way),
            send_sem.at[2, part],
            recv_sem.at[2, part],
        )

    def last_hop(part, way):
        own = pltpu.make_async_copy(
            ready.at[part, hops[2 - way][0]], last_to(part, way), own_sem.at[2, part]
        )
        return last_peers(part, way) + [own]

    def turn(part, way):
        for k in range(N):
            got = select_rows(second_choice[way], near[part, k])
            turned[part, :, k] = got.reshape(N, line_room, LANE)

    def finish(part, way):
        for k in range(2):
            blocks = close[part, 2 * k : 2 * k + 2].reshape(2 * N * line_room, LANE)
            got = select_rows(last_choice[way], blocks)
            at = slice(2 * N * SLOTS * k, 2 * N * SLOTS * (k + 1))
            ready[part, :, at, :] = got.reshape(N, 2 * N * SLOTS, LANE)

    def one_step(step, way, opening=False, closing=False, drained=False):
        groups = []
        if not (closing or drained):
            pack(step + AHEAD)
        if not drained:
            arrived(first_hop(step))
        if not (closing or drained):
            groups.append(first_hop(step + AHEAD))
        if not drained:
            turn(step, way)
            groups.append(second_hop(step, way))
        if not opening:
            arrived(second_hop(step - LAG, way))
            finish(step - LAG, way)
            groups.append(last_hop(step - LAG, way))
        start(*groups)

    one_step(0, 0, opening=True)
    one_step(1, 1, opening=True)
    add_sums(0)
    send_sums(1)

    def two_steps(i, carry):
        for way in range(2):
            one_step(2 * i + way, way)
        for hop in (1, 2):

            @pl.when(i == 2 * hop)
            def _(hop=hop):
                add_sums(hop)
                send_sums(hop + 1)

        return carry

    lax.fori_loop(1, PIECE - 1, two_steps, 0)
    for way in range(2):
        one_step(PARTS - 2 + way, way, closing=True)
    for way in range(2):
        one_step(PARTS + way, way, drained=True)

    for copy in sum_hop(3):
        copy.wait_recv()
    sums_out[...] = sums[3]
    for hop in range(N):
        for copy in sum_hop(hop):
            copy.wait_send()

    def settle(i, carry):
        for way in range(2):
            part = 2 * i + way
            for copy in first_peers(part) + second_peers(part, way):
                copy.wait_send()
            copies = last_hop(part, way)
            arrived(copies)
            for copy in copies[:-1]:
                copy.wait_send()
        return carry

    lax.fori_loop(0, PIECE, settle, 0)


def unpack(lines, sums, file_slot, saved_m, saved_u, checks, full_m, full_u, both, out_sem):
    def move_lines(part, slot, full):
        line = part % PIECE
        if part % 2 == 0:
            for at_y in range(N):
                rows = lines[part, pl.ds(at_y * BLOCK + slot, PLANE, stride=SLOTS), :]
                full[slot, pl.ds(at_y * PIECE + line, PLANE, stride=N * PIECE), :] = rows
        else:
            rows = lines[part, pl.ds(slot, N * PLANE, stride=SLOTS), :]
            full[slot, pl.ds(line, N * PLANE, stride=PIECE), :] = rows

    def out_copy(t, slot):
        full, saved = ((full_m, saved_m), (full_u, saved_u))[t]
        return pltpu.make_async_copy(full.at[slot], saved.at[slot], out_sem.at[t, slot])

    for t, full in enumerate((full_m, full_u)):

        def one_slot(slot, carry, t=t, full=full):
            for part in range(t * PIECE, (t + 1) * PIECE):
                move_lines(part, slot, full)
            out_copy(t, slot).start()
            return carry

        lax.fori_loop(0, SLOTS, one_slot, 0)

    for g in range(N):
        for i in range(2):
            for half in range(2):
                both[2 * g + i : 2 * g + i + 1, half * LANE : (half + 1) * LANE] = sums[
                    g, 2 * i + half : 2 * i + half + 1, :
                ]
    slot_id = lax.broadcasted_iota(jnp.int32, (SPANS, SPANS), 0)
    placing = (file_slot[...] == slot_id).astype(jnp.float32)
    placed = lax.dot_general(
        both[...],
        placing,
        (((1,), (1,)), ((), ())),
        precision=lax.Precision.HIGHEST,
        preferred_element_type=jnp.float32,
    )
    for g in range(N):
        checks[g] = placed[2 * g : 2 * g + 2, :]

    def settle(slot, carry):
        for t in range(2):
            out_copy(t, slot).wait()
        return carry

    lax.fori_loop(0, SLOTS, settle, 0)


SMEM = pl.BlockSpec(memory_space=pltpu.SMEM)
VMEM = pl.BlockSpec(memory_space=pltpu.VMEM)
ANY = pl.BlockSpec(memory_space=pl.ANY)
F32 = jnp.float32


def move(number, master, first, second, rotation, assignment):
    room, line_room = ROOMS[number]
    rows, cols = master.shape
    lines = rows * cols // LANE
    got, sums = pl.pallas_call(
        functools.partial(exchange, room, line_room),
        out_shape=(
            pltpu.VMEM((PARTS, N * BLOCK, LANE), F32),
            jax.ShapeDtypeStruct((N, 8, LANE), F32),
        ),
        in_specs=[ANY, ANY, ANY, VMEM],
        out_specs=(VMEM, VMEM),
        scratch_shapes=[
            pltpu.VMEM((rows, cols), F32),
            pltpu.VMEM((rows, cols), F32),
            pltpu.VMEM((rows, cols), F32),
            pltpu.VMEM((8, SPANS), jnp.int32),
            pltpu.VMEM((2 * lines, LANE), F32),
            pltpu.VMEM((PARTS, N, room, LANE), F32),
            pltpu.VMEM((PARTS, N, room, LANE), F32),
            pltpu.VMEM((PARTS, N, N, line_room, LANE), F32),
            pltpu.VMEM((PARTS, N, N, line_room, LANE), F32),
            pltpu.VMEM((PARTS, N, BLOCK, LANE), F32),
            pltpu.VMEM((N, N, 8, LANE), F32),
            pltpu.VMEM((N, 8, LANE), F32),
            pltpu.SemaphoreType.DMA((3,)),
            pltpu.SemaphoreType.DMA((3, PARTS)),
            pltpu.SemaphoreType.DMA((3, PARTS, N - 1)),
            pltpu.SemaphoreType.DMA((3, PARTS, N - 1)),
            pltpu.SemaphoreType.DMA((N, N - 1)),
            pltpu.SemaphoreType.DMA((N, N - 1)),
        ],
        compiler_params=pltpu.CompilerParams(
            collective_id=number, has_side_effects=True, vmem_limit_bytes=44 << 20
        ),
    )(master, first, second, rotation)
    length = N * PLANE * PIECE
    return pl.pallas_call(
        unpack,
        out_shape=(
            jax.ShapeDtypeStruct((SLOTS, length, LANE), F32),
            jax.ShapeDtypeStruct((SLOTS, length, LANE), F32),
            jax.ShapeDtypeStruct((N, 2, SPANS), F32),
        ),
        in_specs=[VMEM, VMEM, VMEM],
        out_specs=(ANY, ANY, VMEM),
        scratch_shapes=[
            pltpu.VMEM((SLOTS, length, LANE), F32),
            pltpu.VMEM((SLOTS, length, LANE), F32),
            pltpu.VMEM((2 * N, SPANS), F32),
            pltpu.SemaphoreType.DMA((2, SLOTS)),
        ],
        compiler_params=pltpu.CompilerParams(vmem_limit_bytes=16 << 20),
    )(got, sums, assignment)


def shards(master, first, second, rotation, assignment):
    rotation = rotation.reshape(ROUNDS, N * PLANE)
    choice = pl.pallas_call(
        which_room,
        out_shape=jax.ShapeDtypeStruct((1,), jnp.int32),
        in_specs=[VMEM],
        out_specs=SMEM,
        scratch_shapes=[pltpu.VMEM((8, SPANS), jnp.int32)],
        compiler_params=pltpu.CompilerParams(vmem_limit_bytes=4 << 20),
    )(rotation)
    saved_m, saved_u, checks = lax.switch(
        choice[0],
        [functools.partial(move, number) for number in range(len(ROOMS))],
        master[0],
        first[0],
        second[0],
        rotation,
        assignment.reshape(1, SPANS),
    )
    length = N * PLANE * PIECE
    shape = (1, ROUNDS, MOST, length, LANE)
    return saved_m.reshape(shape), saved_u.reshape(shape), checks


def solution(mesh):
    torus = Mesh(mesh.devices.reshape(N, N, N, 2, 2), DP + EXPERT)
    rows = P(EXPERT, DP, None)
    saved = P(EXPERT, DP, None, None, None)
    return jax.shard_map(
        shards,
        mesh=torus,
        in_specs=(rows, rows, rows, P(), P()),
        out_specs=(saved, saved, P()),
        check_vma=False,
    )
```

```python
import functools
import math

import jax
import jax.numpy as jnp
from jax import lax
from jax.experimental import pallas as pl
from jax.experimental.pallas import tpu as pltpu
from jax.sharding import Mesh
from jax.sharding import PartitionSpec as P

LANE = 128
MOST = 3
STEP = 20
BETA_ONE = 0.9
BETA_TWO = 0.95
EPSILON = 1e-08
DP = ("dp_0", "dp_1", "dp_2")
EXPERT = ("expert_0", "expert_1")
MESH = pl.DeviceIdType.MESH

N = 4
ROUNDS = 4
SPANS = 256
PIECE = 7
PARTS = 2 * PIECE
SLOTS = ROUNDS * MOST
PLANE = N * N
BLOCK = PLANE * SLOTS
ROOMS = ((80, 32), (96, 40), (PLANE * SLOTS, N * SLOTS))
AHEAD = 2
LAG = 2


def three_parts(x):
    hi = x.astype(jnp.bfloat16)
    rest = x - hi.astype(jnp.float32)
    mid = rest.astype(jnp.bfloat16)
    low = (rest - mid.astype(jnp.float32)).astype(jnp.bfloat16)
    return hi, mid, low


def select_rows(choice, x):
    parts = jnp.concatenate(three_parts(x), axis=1)
    got = jnp.dot(choice, parts, preferred_element_type=jnp.float32)
    width = x.shape[1]
    return got[:, :width] + got[:, width : 2 * width] + got[:, 2 * width :]


def flat_row(rotation, flat):
    width = rotation.shape[1]
    for r in range(ROUNDS):
        flat[0:1, r * width : (r + 1) * width] = rotation[r : r + 1, :]
    return flat[0:1, :]


def which_room(rotation, choice, flat):
    w = flat_row(rotation, flat)
    x, z, y = w >> 4, (w >> 2) & 3, w & 3
    group = lax.broadcasted_iota(jnp.int32, (PLANE, SPANS), 0)
    in_plane, in_x, in_y = (
        jnp.max(jnp.sum(jnp.where(group == code, 1.0, 0.0), axis=1, keepdims=True))
        for code in (z, z * N + x, z * N + y)
    )
    in_line = jnp.maximum(in_x, in_y)
    misses = [((in_plane > room) | (in_line > line)) for room, line in ROOMS[:-1]]
    choice[0] = sum(miss.astype(jnp.int32) for miss in misses)


def exchange(
    room,
    line_room,
    master,
    first,
    second,
    rotation,
    out,
    sums_out,
    in_m,
    in_one,
    in_two,
    flat,
    flat_lines,
    packed,
    near,
    turned,
    close,
    ready,
    sums,
    part_sum,
    in_sem,
    own_sem,
    send_sem,
    recv_sem,
    s_send,
    s_recv,
    p_send,
    p_recv,
):
    x, z, y = (lax.axis_index(axis) for axis in DP)
    e_0, e_1 = (lax.axis_index(axis) for axis in EXPERT)

    loads = []
    for i, (src, dst) in enumerate(((master, in_m), (first, in_one), (second, in_two))):
        load = pltpu.make_async_copy(src, dst, in_sem.at[i])
        load.start()
        loads.append(load)

    def step_from(place, step):
        return lax.rem(place + step, N)

    def z_peer(s):
        return {"dp_1": step_from(z, s)}

    def x_peer(s):
        return {"dp_0": step_from(x, s)}

    def y_peer(s):
        return {"dp_2": step_from(y, s)}

    def expert_peer(s):
        return {"expert_0": lax.rem(e_0 + s // 2, 2), "expert_1": lax.rem(e_1 + s % 2, 2)}

    def plane_peer(s):
        return {"dp_0": step_from(x, s // N), "dp_2": step_from(y, s % N)}

    hops = ((z, z_peer), (x, x_peer), (y, y_peer), (e_0 * 2 + e_1, expert_peer))
    barrier = pltpu.get_barrier_semaphore()
    others = [peer(s) for peer in (z_peer, expert_peer) for s in range(1, N)]
    others += [plane_peer(s) for s in range(1, PLANE)]
    for other in others:
        pl.semaphore_signal(barrier, inc=1, device_id=other, device_id_type=MESH)

    def to_peers(peer, src, dst, send_sems, recv_sems):
        return [
            pltpu.make_async_remote_copy(
                src_ref=src(s),
                dst_ref=dst,
                send_sem=send_sems.at[s - 1],
                recv_sem=recv_sems.at[s - 1],
                device_id=peer(s),
                device_id_type=MESH,
            )
            for s in (1, 3, 2)
        ]

    def start(*groups):
        for turn in range(N):
            for group in groups:
                group[turn].start()

    def arrived(copies):
        for copy in copies[:-1]:
            copy.wait_recv()
        copies[-1].wait()

    row_id = lax.broadcasted_iota(jnp.int32, (SPANS, SPANS), 0)
    col_id = lax.broadcasted_iota(jnp.int32, (SPANS, SPANS), 1)
    w_row = flat_row(rotation, flat)
    w_col = jnp.sum(jnp.where(row_id == col_id, w_row, 0), axis=1, keepdims=True)
    x_col, z_col, y_col = w_col >> 4, (w_col >> 2) & 3, w_col & 3
    x_row, z_row, y_row = w_row >> 4, (w_row >> 2) & 3, w_row & 3
    same_z = z_col == z_row
    place_row = jnp.sum(jnp.where(same_z & (row_id < col_id), 1, 0), axis=0, keepdims=True)

    def one_hot(count, target):
        ids = lax.broadcasted_iota(jnp.int32, (count, target.shape[1]), 0)
        return (ids == target).astype(jnp.float32).astype(jnp.bfloat16)

    by_plane = one_hot(N * room, z_row * room + place_row)

    rows, per_row = in_m.shape[0], in_m.shape[1] // LANE
    loads[0].wait()
    for col in range(per_row):
        at = slice(col * LANE, (col + 1) * LANE)
        flat_lines[pl.ds(col, rows, stride=per_row), :] = in_m[:, at]

    def piece_lines(part):
        first_line = part + (part // PIECE) * (rows * per_row - PIECE)
        return flat_lines[pl.ds(first_line, SPANS, stride=PIECE), :]

    def pack(part):
        got = select_rows(by_plane, piece_lines(part))
        packed[part] = got.reshape(N, room, LANE)

    def first_peers(part):
        return to_peers(
            z_peer,
            lambda s: packed.at[part, step_from(z, s)],
            near.at[part, z],
            send_sem.at[0, part],
            recv_sem.at[0, part],
        )

    def first_hop(part):
        own = pltpu.make_async_copy(packed.at[part, z], near.at[part, z], own_sem.at[0, part])
        return first_peers(part) + [own]

    pack(0)
    pl.semaphore_wait(barrier, len(others))
    start(first_hop(0))
    for part in range(1, AHEAD):
        pack(part)
        start(first_hop(part))

    corr_one = 1.0 - BETA_ONE**STEP
    corr_two = 1.0 - BETA_TWO**STEP
    loads[1].wait()
    loads[2].wait()
    for col in range(per_row):
        at = slice(col * LANE, (col + 1) * LANE)
        flat_lines[pl.ds(rows * per_row + col, rows, stride=per_row), :] = (in_one[:, at] / corr_one) / (
            jnp.sqrt(in_two[:, at] / corr_two) + EPSILON
        )
    totals = [jnp.zeros((SPANS, LANE), jnp.float32) for _ in range(2)]
    span = lax.broadcasted_iota(jnp.int32, (SPANS, LANE), 0)
    entry = lax.broadcasted_iota(jnp.int32, (SPANS, LANE), 1)
    shift = (5 * rows * ((x * N + z) * N + y)) % 11
    for part in range(PIECE):
        line = span * PIECE + part
        number = 5 * (line // per_row) + 3 * ((line % per_row) * LANE + entry) + shift
        number = number.astype(jnp.float32)
        pattern = number - 11.0 * jnp.floor((number + 0.5) * (1.0 / 11.0))
        weight = 1.0 + pattern * 0.1
        for t in range(2):
            totals[t] += piece_lines(t * PIECE + part) * weight
    scale = 1.0 / math.sqrt(N * PLANE * PIECE * LANE)
    ones = jnp.ones((8, LANE), jnp.float32)
    part_sum[0] = jnp.zeros((8, LANE), jnp.float32)
    for t in range(2):
        row = scale * lax.dot_general(
            ones,
            totals[t],
            (((1,), (1,)), ((), ())),
            precision=lax.Precision.HIGHEST,
            preferred_element_type=jnp.float32,
        )
        for half in range(2):
            part_sum[0, 2 * t + half : 2 * t + half + 1, :] = row[
                0:1, half * LANE : (half + 1) * LANE
            ]

    def sum_hop(hop):
        place, peer = hops[hop]
        return to_peers(
            peer,
            lambda s: part_sum.at[hop],
            sums.at[hop, place],
            s_send.at[hop],
            s_recv.at[hop],
        )

    def send_sums(hop):
        sums[hop, hops[hop][0]] = part_sum[hop]
        for copy in sum_hop(hop):
            copy.start()

    def add_sums(hop):
        for copy in sum_hop(hop):
            copy.wait_recv()
        part_sum[hop + 1] = sums[hop, 0] + sums[hop, 1] + sums[hop, 2] + sums[hop, 3]

    send_sums(0)

    before = col_id < row_id

    def count(same):
        return jnp.sum(jnp.where(same & before, 1, 0), axis=1, keepdims=True)

    place_col = count(same_z)
    in_round = (row_id >> 6) == (col_id >> 6)
    slot_col = count((w_col == w_row) & in_round)
    slot_col += (lax.broadcasted_iota(jnp.int32, (SPANS, 1), 0) >> 6) * MOST

    def found(at, value):
        return jnp.sum(jnp.where(at, value + 1, 0), axis=0, keepdims=True) - 1

    in_plane = z_col == z
    plane_at = lax.broadcasted_iota(jnp.int32, (1, room), 1)
    line_at = lax.broadcasted_iota(jnp.int32, (1, 2 * N * line_room), 1)
    source = jnp.zeros_like(line_at)
    for k in range(1, 2 * N):
        source += jnp.where(line_at >= k * line_room, 1, 0)
    line_at = line_at - source * line_room
    second_choice, last_choice = [], []
    for line_col, line_row, own, end_col in (
        (x_col, x_row, x, y_col),
        (y_col, y_row, y, x_col),
    ):
        in_line = count(same_z & (line_col == line_row))
        target = found(in_plane & (place_col == plane_at), line_col * line_room + in_line)
        second_choice.append(one_hot(N * line_room, target))
        here = in_plane & (line_col == own) & (in_line == line_at)
        target = found(here, end_col * (2 * N * SLOTS) + slot_col)
        target += jnp.where(target >= 0, source * SLOTS, 0)
        last_choice.append(one_hot(2 * N * N * SLOTS, target))

    def second_to(part, way):
        place = hops[1 + way][0]
        return close.at[part, place] if way == 0 else close.at[part, :, place]

    def second_peers(part, way):
        place, peer = hops[1 + way]
        return to_peers(
            peer,
            lambda s: turned.at[part, step_from(place, s)],
            second_to(part, way),
            send_sem.at[1, part],
            recv_sem.at[1, part],
        )

    def second_hop(part, way):
        own = pltpu.make_async_copy(
            turned.at[part, hops[1 + way][0]], second_to(part, way), own_sem.at[1, part]
        )
        return second_peers(part, way) + [own]

    def last_to(part, way):
        place = hops[2 - way][0]
        return out.at[part, pl.ds(pl.multiple_of(place * BLOCK, 8), BLOCK)]

    def last_peers(part, way):
        place, peer = hops[2 - way]
        return to_peers(
            peer,
            lambda s: ready.at[part, step_from(place, s)],
            last_to(part, way),
            send_sem.at[2, part],
            recv_sem.at[2, part],
        )

    def last_hop(part, way):
        own = pltpu.make_async_copy(
            ready.at[part, hops[2 - way][0]], last_to(part, way), own_sem.at[2, part]
        )
        return last_peers(part, way) + [own]

    def turn(part, way):
        for k in range(N):
            got = select_rows(second_choice[way], near[part, k])
            turned[part, :, k] = got.reshape(N, line_room, LANE)

    def finish(part, way):
        for k in range(2):
            blocks = close[part, 2 * k : 2 * k + 2].reshape(2 * N * line_room, LANE)
            got = select_rows(last_choice[way], blocks)
            at = slice(2 * N * SLOTS * k, 2 * N * SLOTS * (k + 1))
            ready[part, :, at, :] = got.reshape(N, 2 * N * SLOTS, LANE)

    final = PARTS - 1
    plane_at = lax.broadcasted_iota(jnp.int32, (1, 2 * room), 1)
    upper = plane_at >= room
    here = in_plane & (place_col == jnp.where(upper, plane_at - room, plane_at))
    target = found(here, (x_col * N + y_col) * (2 * SLOTS) + slot_col)
    target += jnp.where((target >= 0) & upper, SLOTS, 0)
    final_choice = one_hot(2 * SLOTS * PLANE, target)
    share = N * SLOTS

    def share_at(index):
        return pl.ds(pl.multiple_of(index * share, 8), share)

    def direct_peers():
        return [
            pltpu.make_async_remote_copy(
                src_ref=ready.at[final, step_from(x, s // N), share_at(step_from(y, s % N))],
                dst_ref=out.at[final, share_at(y * N + x)],
                send_sem=p_send.at[s - 1],
                recv_sem=p_recv.at[s - 1],
                device_id=plane_peer(s),
                device_id_type=MESH,
            )
            for s in range(1, PLANE)
        ]

    def direct():
        own = pltpu.make_async_copy(
            ready.at[final, x, share_at(y)], out.at[final, share_at(y * N + x)], own_sem.at[2, final]
        )
        return direct_peers() + [own]

    def finish_direct():
        for k in range(2):
            blocks = near[final, 2 * k : 2 * k + 2].reshape(2 * room, LANE)
            got = select_rows(final_choice, blocks).reshape(N, N, 2 * SLOTS, LANE)
            for to_y in range(N):
                first_row = to_y * share + 2 * SLOTS * k
                ready[final, :, first_row : first_row + 2 * SLOTS, :] = got[:, to_y]

    def one_step(step, way, opening=False, closing=False, drained=False):
        groups = []
        if not (closing or drained):
            pack(step + AHEAD)
        if not drained:
            arrived(first_hop(step))
        if not (closing or drained):
            groups.append(first_hop(step + AHEAD))
        if not drained:
            turn(step, way)
            groups.append(second_hop(step, way))
        if not opening:
            arrived(second_hop(step - LAG, way))
            finish(step - LAG, way)
            groups.append(last_hop(step - LAG, way))
        start(*groups)

    one_step(0, 0, opening=True)
    one_step(1, 1, opening=True)
    add_sums(0)
    send_sums(1)

    def two_steps(i, carry):
        for way in range(2):
            one_step(2 * i + way, way)
        for hop in (1, 2):

            @pl.when(i == 2 * hop)
            def _(hop=hop):
                add_sums(hop)
                send_sums(hop + 1)

        return carry

    lax.fori_loop(1, PIECE - 1, two_steps, 0)
    one_step(final - 1, 0, closing=True)
    arrived(first_hop(final))
    finish_direct()
    for copy in direct():
        copy.start()
    one_step(final + LAG - 2, 1, drained=True)
    one_step(final + LAG - 1, 0, drained=True)

    for copy in sum_hop(3):
        copy.wait_recv()
    sums_out[...] = sums[3]
    for hop in range(N):
        for copy in sum_hop(hop):
            copy.wait_send()

    def settle_part(part, way):
        for copy in first_peers(part) + second_peers(part, way):
            copy.wait_send()
        copies = last_hop(part, way)
        arrived(copies)
        for copy in copies[:-1]:
            copy.wait_send()

    def settle(i, carry):
        for way in range(2):
            settle_part(2 * i + way, way)
        return carry

    lax.fori_loop(0, PIECE - 1, settle, 0)
    settle_part(final - 1, 0)
    for copy in first_peers(final):
        copy.wait_send()
    copies = direct()
    arrived(copies)
    for copy in copies[:-1]:
        copy.wait_send()


def unpack(lines, sums, file_slot, saved_m, saved_u, checks, full_m, full_u, both, out_sem):
    def move_lines(part, slot, full):
        line = part % PIECE
        if part % 2 == 0 or part == PARTS - 1:
            for at_y in range(N):
                rows = lines[part, pl.ds(at_y * BLOCK + slot, PLANE, stride=SLOTS), :]
                full[slot, pl.ds(at_y * PIECE + line, PLANE, stride=N * PIECE), :] = rows
        else:
            rows = lines[part, pl.ds(slot, N * PLANE, stride=SLOTS), :]
            full[slot, pl.ds(line, N * PLANE, stride=PIECE), :] = rows

    def out_copy(t, slot):
        full, saved = ((full_m, saved_m), (full_u, saved_u))[t]
        return pltpu.make_async_copy(full.at[slot], saved.at[slot], out_sem.at[t, slot])

    for t, full in enumerate((full_m, full_u)):

        def one_slot(slot, carry, t=t, full=full):
            for part in range(t * PIECE, (t + 1) * PIECE):
                move_lines(part, slot, full)
            out_copy(t, slot).start()
            return carry

        lax.fori_loop(0, SLOTS, one_slot, 0)

    for g in range(N):
        for i in range(2):
            for half in range(2):
                both[2 * g + i : 2 * g + i + 1, half * LANE : (half + 1) * LANE] = sums[
                    g, 2 * i + half : 2 * i + half + 1, :
                ]
    slot_id = lax.broadcasted_iota(jnp.int32, (SPANS, SPANS), 0)
    placing = (file_slot[...] == slot_id).astype(jnp.float32)
    placed = lax.dot_general(
        both[...],
        placing,
        (((1,), (1,)), ((), ())),
        precision=lax.Precision.HIGHEST,
        preferred_element_type=jnp.float32,
    )
    for g in range(N):
        checks[g] = placed[2 * g : 2 * g + 2, :]

    def settle(slot, carry):
        for t in range(2):
            out_copy(t, slot).wait()
        return carry

    lax.fori_loop(0, SLOTS, settle, 0)


SMEM = pl.BlockSpec(memory_space=pltpu.SMEM)
VMEM = pl.BlockSpec(memory_space=pltpu.VMEM)
ANY = pl.BlockSpec(memory_space=pl.ANY)
F32 = jnp.float32


def move(number, master, first, second, rotation, assignment):
    room, line_room = ROOMS[number]
    rows, cols = master.shape
    lines = rows * cols // LANE
    got, sums = pl.pallas_call(
        functools.partial(exchange, room, line_room),
        out_shape=(
            pltpu.VMEM((PARTS, N * BLOCK, LANE), F32),
            jax.ShapeDtypeStruct((N, 8, LANE), F32),
        ),
        in_specs=[ANY, ANY, ANY, VMEM],
        out_specs=(VMEM, VMEM),
        scratch_shapes=[
            pltpu.VMEM((rows, cols), F32),
            pltpu.VMEM((rows, cols), F32),
            pltpu.VMEM((rows, cols), F32),
            pltpu.VMEM((8, SPANS), jnp.int32),
            pltpu.VMEM((2 * lines, LANE), F32),
            pltpu.VMEM((PARTS, N, room, LANE), F32),
            pltpu.VMEM((PARTS, N, room, LANE), F32),
            pltpu.VMEM((PARTS, N, N, line_room, LANE), F32),
            pltpu.VMEM((PARTS, N, N, line_room, LANE), F32),
            pltpu.VMEM((PARTS, N, BLOCK, LANE), F32),
            pltpu.VMEM((N, N, 8, LANE), F32),
            pltpu.VMEM((N, 8, LANE), F32),
            pltpu.SemaphoreType.DMA((3,)),
            pltpu.SemaphoreType.DMA((3, PARTS)),
            pltpu.SemaphoreType.DMA((3, PARTS, N - 1)),
            pltpu.SemaphoreType.DMA((3, PARTS, N - 1)),
            pltpu.SemaphoreType.DMA((N, N - 1)),
            pltpu.SemaphoreType.DMA((N, N - 1)),
            pltpu.SemaphoreType.DMA((PLANE - 1,)),
            pltpu.SemaphoreType.DMA((PLANE - 1,)),
        ],
        compiler_params=pltpu.CompilerParams(
            collective_id=number, has_side_effects=True, vmem_limit_bytes=44 << 20
        ),
    )(master, first, second, rotation)
    length = N * PLANE * PIECE
    return pl.pallas_call(
        unpack,
        out_shape=(
            jax.ShapeDtypeStruct((SLOTS, length, LANE), F32),
            jax.ShapeDtypeStruct((SLOTS, length, LANE), F32),
            jax.ShapeDtypeStruct((N, 2, SPANS), F32),
        ),
        in_specs=[VMEM, VMEM, VMEM],
        out_specs=(ANY, ANY, VMEM),
        scratch_shapes=[
            pltpu.VMEM((SLOTS, length, LANE), F32),
            pltpu.VMEM((SLOTS, length, LANE), F32),
            pltpu.VMEM((2 * N, SPANS), F32),
            pltpu.SemaphoreType.DMA((2, SLOTS)),
        ],
        compiler_params=pltpu.CompilerParams(vmem_limit_bytes=16 << 20),
    )(got, sums, assignment)


def shards(master, first, second, rotation, assignment):
    rotation = rotation.reshape(ROUNDS, N * PLANE)
    choice = pl.pallas_call(
        which_room,
        out_shape=jax.ShapeDtypeStruct((1,), jnp.int32),
        in_specs=[VMEM],
        out_specs=SMEM,
        scratch_shapes=[pltpu.VMEM((8, SPANS), jnp.int32)],
        compiler_params=pltpu.CompilerParams(vmem_limit_bytes=4 << 20),
    )(rotation)
    saved_m, saved_u, checks = lax.switch(
        choice[0],
        [functools.partial(move, number) for number in range(len(ROOMS))],
        master[0],
        first[0],
        second[0],
        rotation,
        assignment.reshape(1, SPANS),
    )
    length = N * PLANE * PIECE
    shape = (1, ROUNDS, MOST, length, LANE)
    return saved_m.reshape(shape), saved_u.reshape(shape), checks


def solution(mesh):
    torus = Mesh(mesh.devices.reshape(N, N, N, 2, 2), DP + EXPERT)
    rows = P(EXPERT, DP, None)
    saved = P(EXPERT, DP, None, None, None)
    return jax.shard_map(
        shards,
        mesh=torus,
        in_specs=(rows, rows, rows, P(), P()),
        out_specs=(saved, saved, P()),
        check_vma=False,
    )
```

```python
import functools
import math

import jax
import jax.numpy as jnp
from jax import lax
from jax.experimental import pallas as pl
from jax.experimental.pallas import tpu as pltpu
from jax.sharding import Mesh
from jax.sharding import PartitionSpec as P

LANE = 128
MOST = 3
STEP = 20
BETA_ONE = 0.9
BETA_TWO = 0.95
EPSILON = 1e-08
DP = ("dp_0", "dp_1", "dp_2")
EXPERT = ("expert_0", "expert_1")
MESH = pl.DeviceIdType.MESH

N = 4
ROUNDS = 4
SPANS = 256
PIECE = 7
PARTS = 2 * PIECE
SLOTS = ROUNDS * MOST
PLANE = N * N
BLOCK = PLANE * SLOTS
ROOMS = ((80, 32), (96, 40), (PLANE * SLOTS, N * SLOTS))
AHEAD = 2
LAG = 2


def three_parts(x):
    hi = x.astype(jnp.bfloat16)
    rest = x - hi.astype(jnp.float32)
    mid = rest.astype(jnp.bfloat16)
    low = (rest - mid.astype(jnp.float32)).astype(jnp.bfloat16)
    return hi, mid, low


def select_rows(choice, x):
    parts = jnp.concatenate(three_parts(x), axis=1)
    got = jnp.dot(choice, parts, preferred_element_type=jnp.float32)
    width = x.shape[1]
    return got[:, :width] + got[:, width : 2 * width] + got[:, 2 * width :]


def flat_row(rotation, flat):
    width = rotation.shape[1]
    for r in range(ROUNDS):
        flat[0:1, r * width : (r + 1) * width] = rotation[r : r + 1, :]
    return flat[0:1, :]


def which_room(rotation, choice, flat):
    w = flat_row(rotation, flat)
    x, z, y = w >> 4, (w >> 2) & 3, w & 3
    group = lax.broadcasted_iota(jnp.int32, (PLANE, SPANS), 0)
    in_plane, in_x, in_y = (
        jnp.max(jnp.sum(jnp.where(group == code, 1.0, 0.0), axis=1, keepdims=True))
        for code in (z, z * N + x, z * N + y)
    )
    in_line = jnp.maximum(in_x, in_y)
    misses = [((in_plane > room) | (in_line > line)) for room, line in ROOMS[:-1]]
    choice[0] = sum(miss.astype(jnp.int32) for miss in misses)


def exchange(
    room,
    line_room,
    master,
    first,
    second,
    rotation,
    out,
    sums_out,
    in_m,
    in_one,
    in_two,
    flat,
    flat_lines,
    packed,
    near,
    turned,
    close,
    ready,
    sums,
    part_sum,
    in_sem,
    own_sem,
    send_sem,
    recv_sem,
    s_send,
    s_recv,
    p_send,
    p_recv,
):
    x, z, y = (lax.axis_index(axis) for axis in DP)
    e_0, e_1 = (lax.axis_index(axis) for axis in EXPERT)

    loads = []
    for i, (src, dst) in enumerate(((master, in_m), (first, in_one), (second, in_two))):
        load = pltpu.make_async_copy(src, dst, in_sem.at[i])
        load.start()
        loads.append(load)

    def step_from(place, step):
        return lax.rem(place + step, N)

    def z_peer(s):
        return {"dp_1": step_from(z, s)}

    def x_peer(s):
        return {"dp_0": step_from(x, s)}

    def y_peer(s):
        return {"dp_2": step_from(y, s)}

    def expert_peer(s):
        return {"expert_0": lax.rem(e_0 + s // 2, 2), "expert_1": lax.rem(e_1 + s % 2, 2)}

    def plane_peer(s):
        return {"dp_0": step_from(x, s // N), "dp_2": step_from(y, s % N)}

    hops = ((z, z_peer), (x, x_peer), (y, y_peer), (e_0 * 2 + e_1, expert_peer))
    barrier = pltpu.get_barrier_semaphore()
    others = [peer(s) for peer in (z_peer, expert_peer) for s in range(1, N)]
    others += [plane_peer(s) for s in range(1, PLANE)]
    for other in others:
        pl.semaphore_signal(barrier, inc=1, device_id=other, device_id_type=MESH)

    def to_peers(peer, src, dst, send_sems, recv_sems):
        return [
            pltpu.make_async_remote_copy(
                src_ref=src(s),
                dst_ref=dst,
                send_sem=send_sems.at[s - 1],
                recv_sem=recv_sems.at[s - 1],
                device_id=peer(s),
                device_id_type=MESH,
            )
            for s in (1, 3, 2)
        ]

    def start(*groups):
        for turn in range(N):
            for group in groups:
                group[turn].start()

    def arrived(copies):
        for copy in copies[:-1]:
            copy.wait_recv()
        copies[-1].wait()

    row_id = lax.broadcasted_iota(jnp.int32, (SPANS, SPANS), 0)
    col_id = lax.broadcasted_iota(jnp.int32, (SPANS, SPANS), 1)
    w_row = flat_row(rotation, flat)
    w_col = jnp.sum(jnp.where(row_id == col_id, w_row, 0), axis=1, keepdims=True)
    x_col, z_col, y_col = w_col >> 4, (w_col >> 2) & 3, w_col & 3
    x_row, z_row, y_row = w_row >> 4, (w_row >> 2) & 3, w_row & 3
    same_z = z_col == z_row
    place_row = jnp.sum(jnp.where(same_z & (row_id < col_id), 1, 0), axis=0, keepdims=True)

    def one_hot(count, target):
        ids = lax.broadcasted_iota(jnp.int32, (count, target.shape[1]), 0)
        return (ids == target).astype(jnp.float32).astype(jnp.bfloat16)

    by_plane = one_hot(N * room, z_row * room + place_row)

    rows, per_row = in_m.shape[0], in_m.shape[1] // LANE
    loads[0].wait()
    for col in range(per_row):
        at = slice(col * LANE, (col + 1) * LANE)
        flat_lines[pl.ds(col, rows, stride=per_row), :] = in_m[:, at]

    def piece_lines(part):
        first_line = part + (part // PIECE) * (rows * per_row - PIECE)
        return flat_lines[pl.ds(first_line, SPANS, stride=PIECE), :]

    def pack(part):
        got = select_rows(by_plane, piece_lines(part))
        packed[part] = got.reshape(N, room, LANE)

    def first_peers(part):
        return to_peers(
            z_peer,
            lambda s: packed.at[part, step_from(z, s)],
            near.at[part, z],
            send_sem.at[0, part],
            recv_sem.at[0, part],
        )

    def first_hop(part):
        own = pltpu.make_async_copy(packed.at[part, z], near.at[part, z], own_sem.at[0, part])
        return first_peers(part) + [own]

    pack(0)
    pl.semaphore_wait(barrier, len(others))
    start(first_hop(0))
    for part in range(1, AHEAD):
        pack(part)
        start(first_hop(part))

    corr_one = 1.0 - BETA_ONE**STEP
    corr_two = 1.0 - BETA_TWO**STEP
    loads[1].wait()
    loads[2].wait()
    for col in range(per_row):
        at = slice(col * LANE, (col + 1) * LANE)
        flat_lines[pl.ds(rows * per_row + col, rows, stride=per_row), :] = (in_one[:, at] / corr_one) / (
            jnp.sqrt(in_two[:, at] / corr_two) + EPSILON
        )
    totals = [jnp.zeros((SPANS, LANE), jnp.float32) for _ in range(2)]
    span = lax.broadcasted_iota(jnp.int32, (SPANS, LANE), 0)
    entry = lax.broadcasted_iota(jnp.int32, (SPANS, LANE), 1)
    shift = (5 * rows * ((x * N + z) * N + y)) % 11
    for part in range(PIECE):
        line = span * PIECE + part
        number = 5 * (line // per_row) + 3 * ((line % per_row) * LANE + entry) + shift
        number = number.astype(jnp.float32)
        pattern = number - 11.0 * jnp.floor((number + 0.5) * (1.0 / 11.0))
        weight = 1.0 + pattern * 0.1
        for t in range(2):
            totals[t] += piece_lines(t * PIECE + part) * weight
    scale = 1.0 / math.sqrt(N * PLANE * PIECE * LANE)
    ones = jnp.ones((8, LANE), jnp.float32)
    part_sum[0] = jnp.zeros((8, LANE), jnp.float32)
    for t in range(2):
        row = scale * lax.dot_general(
            ones,
            totals[t],
            (((1,), (1,)), ((), ())),
            precision=lax.Precision.HIGHEST,
            preferred_element_type=jnp.float32,
        )
        for half in range(2):
            part_sum[0, 2 * t + half : 2 * t + half + 1, :] = row[
                0:1, half * LANE : (half + 1) * LANE
            ]

    def sum_hop(hop):
        place, peer = hops[hop]
        return to_peers(
            peer,
            lambda s: part_sum.at[hop],
            sums.at[hop, place],
            s_send.at[hop],
            s_recv.at[hop],
        )

    def send_sums(hop):
        sums[hop, hops[hop][0]] = part_sum[hop]
        for copy in sum_hop(hop):
            copy.start()

    def add_sums(hop):
        for copy in sum_hop(hop):
            copy.wait_recv()
        part_sum[hop + 1] = sums[hop, 0] + sums[hop, 1] + sums[hop, 2] + sums[hop, 3]

    send_sums(0)

    before = col_id < row_id

    def count(same):
        return jnp.sum(jnp.where(same & before, 1, 0), axis=1, keepdims=True)

    place_col = count(same_z)
    in_round = (row_id >> 6) == (col_id >> 6)
    slot_col = count((w_col == w_row) & in_round)
    slot_col += (lax.broadcasted_iota(jnp.int32, (SPANS, 1), 0) >> 6) * MOST

    def found(at, value):
        return jnp.sum(jnp.where(at, value + 1, 0), axis=0, keepdims=True) - 1

    in_plane = z_col == z
    plane_at = lax.broadcasted_iota(jnp.int32, (1, room), 1)
    line_at = lax.broadcasted_iota(jnp.int32, (1, 2 * N * line_room), 1)
    source = jnp.zeros_like(line_at)
    for k in range(1, 2 * N):
        source += jnp.where(line_at >= k * line_room, 1, 0)
    line_at = line_at - source * line_room
    second_choice, last_choice = [], []
    for line_col, line_row, own, end_col in (
        (x_col, x_row, x, y_col),
        (y_col, y_row, y, x_col),
    ):
        in_line = count(same_z & (line_col == line_row))
        target = found(in_plane & (place_col == plane_at), line_col * line_room + in_line)
        second_choice.append(one_hot(N * line_room, target))
        here = in_plane & (line_col == own) & (in_line == line_at)
        target = found(here, end_col * (2 * N * SLOTS) + slot_col)
        target += jnp.where(target >= 0, source * SLOTS, 0)
        last_choice.append(one_hot(2 * N * N * SLOTS, target))

    def second_to(part, way):
        place = hops[1 + way][0]
        return close.at[part, place] if way == 0 else close.at[part, :, place]

    def second_peers(part, way):
        place, peer = hops[1 + way]
        return to_peers(
            peer,
            lambda s: turned.at[part, step_from(place, s)],
            second_to(part, way),
            send_sem.at[1, part],
            recv_sem.at[1, part],
        )

    def second_hop(part, way):
        own = pltpu.make_async_copy(
            turned.at[part, hops[1 + way][0]], second_to(part, way), own_sem.at[1, part]
        )
        return second_peers(part, way) + [own]

    def last_to(part, way):
        place = hops[2 - way][0]
        return out.at[part, pl.ds(pl.multiple_of(place * BLOCK, 8), BLOCK)]

    def last_peers(part, way):
        place, peer = hops[2 - way]
        return to_peers(
            peer,
            lambda s: ready.at[part, step_from(place, s)],
            last_to(part, way),
            send_sem.at[2, part],
            recv_sem.at[2, part],
        )

    def last_hop(part, way):
        own = pltpu.make_async_copy(
            ready.at[part, hops[2 - way][0]], last_to(part, way), own_sem.at[2, part]
        )
        return last_peers(part, way) + [own]

    def turn(part, way):
        for k in range(N):
            got = select_rows(second_choice[way], near[part, k])
            turned[part, :, k] = got.reshape(N, line_room, LANE)

    def finish(part, way):
        for k in range(2):
            blocks = close[part, 2 * k : 2 * k + 2].reshape(2 * N * line_room, LANE)
            got = select_rows(last_choice[way], blocks)
            at = slice(2 * N * SLOTS * k, 2 * N * SLOTS * (k + 1))
            ready[part, :, at, :] = got.reshape(N, 2 * N * SLOTS, LANE)

    final = PARTS - 1
    plane_at = lax.broadcasted_iota(jnp.int32, (1, 2 * room), 1)
    upper = plane_at >= room
    here = in_plane & (place_col == jnp.where(upper, plane_at - room, plane_at))
    target = found(here, (x_col * N + y_col) * (2 * SLOTS) + slot_col)
    target += jnp.where((target >= 0) & upper, SLOTS, 0)
    final_choice = one_hot(2 * SLOTS * PLANE, target)
    share = N * SLOTS

    def share_at(index):
        return pl.ds(pl.multiple_of(index * share, 8), share)

    def direct_peers():
        return [
            pltpu.make_async_remote_copy(
                src_ref=ready.at[final, step_from(x, s // N), share_at(step_from(y, s % N))],
                dst_ref=out.at[final, share_at(y * N + x)],
                send_sem=p_send.at[s - 1],
                recv_sem=p_recv.at[s - 1],
                device_id=plane_peer(s),
                device_id_type=MESH,
            )
            for s in range(1, PLANE)
        ]

    def direct():
        own = pltpu.make_async_copy(
            ready.at[final, x, share_at(y)], out.at[final, share_at(y * N + x)], own_sem.at[2, final]
        )
        return direct_peers() + [own]

    def finish_direct():
        for k in range(2):
            blocks = near[final, 2 * k : 2 * k + 2].reshape(2 * room, LANE)
            got = select_rows(final_choice, blocks).reshape(N, N, 2 * SLOTS, LANE)
            for to_y in range(N):
                first_row = to_y * share + 2 * SLOTS * k
                ready[final, :, first_row : first_row + 2 * SLOTS, :] = got[:, to_y]

    def one_step(step, way, opening=False, closing=False, drained=False):
        if not (closing or drained):
            pack(step + AHEAD)
        if not opening:
            arrived(second_hop(step - LAG, way))
            finish(step - LAG, way)
            start(last_hop(step - LAG, way))
        groups = []
        if not drained:
            arrived(first_hop(step))
        if not (closing or drained):
            groups.append(first_hop(step + AHEAD))
        if not drained:
            turn(step, way)
            groups.append(second_hop(step, way))
        start(*groups)

    one_step(0, 0, opening=True)
    one_step(1, 1, opening=True)
    add_sums(0)
    send_sums(1)

    def two_steps(i, carry):
        for way in range(2):
            one_step(2 * i + way, way)
        for hop in (1, 2):

            @pl.when(i == 2 * hop)
            def _(hop=hop):
                add_sums(hop)
                send_sums(hop + 1)

        return carry

    lax.fori_loop(1, PIECE - 1, two_steps, 0)
    one_step(final - 1, 0, closing=True)
    one_step(final, 1, drained=True)
    arrived(first_hop(final))
    finish_direct()
    for copy in direct():
        copy.start()
    one_step(final + 1, 0, drained=True)

    for copy in sum_hop(3):
        copy.wait_recv()
    sums_out[...] = sums[3]
    for hop in range(N):
        for copy in sum_hop(hop):
            copy.wait_send()

    def settle_part(part, way):
        for copy in first_peers(part) + second_peers(part, way):
            copy.wait_send()
        copies = last_hop(part, way)
        arrived(copies)
        for copy in copies[:-1]:
            copy.wait_send()

    def settle(i, carry):
        for way in range(2):
            settle_part(2 * i + way, way)
        return carry

    lax.fori_loop(0, PIECE - 1, settle, 0)
    settle_part(final - 1, 0)
    for copy in first_peers(final):
        copy.wait_send()
    copies = direct()
    arrived(copies)
    for copy in copies[:-1]:
        copy.wait_send()


def unpack(lines, sums, file_slot, saved_m, saved_u, checks, full_m, full_u, both, out_sem):
    def move_lines(part, slot, full):
        line = part % PIECE
        if part % 2 == 0 or part == PARTS - 1:
            for at_y in range(N):
                rows = lines[part, pl.ds(at_y * BLOCK + slot, PLANE, stride=SLOTS), :]
                full[slot, pl.ds(at_y * PIECE + line, PLANE, stride=N * PIECE), :] = rows
        else:
            rows = lines[part, pl.ds(slot, N * PLANE, stride=SLOTS), :]
            full[slot, pl.ds(line, N * PLANE, stride=PIECE), :] = rows

    def out_copy(t, slot):
        full, saved = ((full_m, saved_m), (full_u, saved_u))[t]
        return pltpu.make_async_copy(full.at[slot], saved.at[slot], out_sem.at[t, slot])

    for t, full in enumerate((full_m, full_u)):

        def one_slot(slot, carry, t=t, full=full):
            for part in range(t * PIECE, (t + 1) * PIECE):
                move_lines(part, slot, full)
            out_copy(t, slot).start()
            return carry

        lax.fori_loop(0, SLOTS, one_slot, 0)

    for g in range(N):
        for i in range(2):
            for half in range(2):
                both[2 * g + i : 2 * g + i + 1, half * LANE : (half + 1) * LANE] = sums[
                    g, 2 * i + half : 2 * i + half + 1, :
                ]
    slot_id = lax.broadcasted_iota(jnp.int32, (SPANS, SPANS), 0)
    placing = (file_slot[...] == slot_id).astype(jnp.float32)
    placed = lax.dot_general(
        both[...],
        placing,
        (((1,), (1,)), ((), ())),
        precision=lax.Precision.HIGHEST,
        preferred_element_type=jnp.float32,
    )
    for g in range(N):
        checks[g] = placed[2 * g : 2 * g + 2, :]

    def settle(slot, carry):
        for t in range(2):
            out_copy(t, slot).wait()
        return carry

    lax.fori_loop(0, SLOTS, settle, 0)


SMEM = pl.BlockSpec(memory_space=pltpu.SMEM)
VMEM = pl.BlockSpec(memory_space=pltpu.VMEM)
ANY = pl.BlockSpec(memory_space=pl.ANY)
F32 = jnp.float32


def move(number, master, first, second, rotation, assignment):
    room, line_room = ROOMS[number]
    rows, cols = master.shape
    lines = rows * cols // LANE
    got, sums = pl.pallas_call(
        functools.partial(exchange, room, line_room),
        out_shape=(
            pltpu.VMEM((PARTS, N * BLOCK, LANE), F32),
            jax.ShapeDtypeStruct((N, 8, LANE), F32),
        ),
        in_specs=[ANY, ANY, ANY, VMEM],
        out_specs=(VMEM, VMEM),
        scratch_shapes=[
            pltpu.VMEM((rows, cols), F32),
            pltpu.VMEM((rows, cols), F32),
            pltpu.VMEM((rows, cols), F32),
            pltpu.VMEM((8, SPANS), jnp.int32),
            pltpu.VMEM((2 * lines, LANE), F32),
            pltpu.VMEM((PARTS, N, room, LANE), F32),
            pltpu.VMEM((PARTS, N, room, LANE), F32),
            pltpu.VMEM((PARTS, N, N, line_room, LANE), F32),
            pltpu.VMEM((PARTS, N, N, line_room, LANE), F32),
            pltpu.VMEM((PARTS, N, BLOCK, LANE), F32),
            pltpu.VMEM((N, N, 8, LANE), F32),
            pltpu.VMEM((N, 8, LANE), F32),
            pltpu.SemaphoreType.DMA((3,)),
            pltpu.SemaphoreType.DMA((3, PARTS)),
            pltpu.SemaphoreType.DMA((3, PARTS, N - 1)),
            pltpu.SemaphoreType.DMA((3, PARTS, N - 1)),
            pltpu.SemaphoreType.DMA((N, N - 1)),
            pltpu.SemaphoreType.DMA((N, N - 1)),
            pltpu.SemaphoreType.DMA((PLANE - 1,)),
            pltpu.SemaphoreType.DMA((PLANE - 1,)),
        ],
        compiler_params=pltpu.CompilerParams(
            collective_id=number, has_side_effects=True, vmem_limit_bytes=44 << 20
        ),
    )(master, first, second, rotation)
    length = N * PLANE * PIECE
    return pl.pallas_call(
        unpack,
        out_shape=(
            jax.ShapeDtypeStruct((SLOTS, length, LANE), F32),
            jax.ShapeDtypeStruct((SLOTS, length, LANE), F32),
            jax.ShapeDtypeStruct((N, 2, SPANS), F32),
        ),
        in_specs=[VMEM, VMEM, VMEM],
        out_specs=(ANY, ANY, VMEM),
        scratch_shapes=[
            pltpu.VMEM((SLOTS, length, LANE), F32),
            pltpu.VMEM((SLOTS, length, LANE), F32),
            pltpu.VMEM((2 * N, SPANS), F32),
            pltpu.SemaphoreType.DMA((2, SLOTS)),
        ],
        compiler_params=pltpu.CompilerParams(vmem_limit_bytes=16 << 20),
    )(got, sums, assignment)


def shards(master, first, second, rotation, assignment):
    rotation = rotation.reshape(ROUNDS, N * PLANE)
    choice = pl.pallas_call(
        which_room,
        out_shape=jax.ShapeDtypeStruct((1,), jnp.int32),
        in_specs=[VMEM],
        out_specs=SMEM,
        scratch_shapes=[pltpu.VMEM((8, SPANS), jnp.int32)],
        compiler_params=pltpu.CompilerParams(vmem_limit_bytes=4 << 20),
    )(rotation)
    saved_m, saved_u, checks = lax.switch(
        choice[0],
        [functools.partial(move, number) for number in range(len(ROOMS))],
        master[0],
        first[0],
        second[0],
        rotation,
        assignment.reshape(1, SPANS),
    )
    length = N * PLANE * PIECE
    shape = (1, ROUNDS, MOST, length, LANE)
    return saved_m.reshape(shape), saved_u.reshape(shape), checks


def solution(mesh):
    torus = Mesh(mesh.devices.reshape(N, N, N, 2, 2), DP + EXPERT)
    rows = P(EXPERT, DP, None)
    saved = P(EXPERT, DP, None, None, None)
    return jax.shard_map(
        shards,
        mesh=torus,
        in_specs=(rows, rows, rows, P(), P()),
        out_specs=(saved, saved, P()),
        check_vma=False,
    )
```
